32 devices in a mesh: gx: 4 (over y, x), gy: 2 (over core), gz: 4 (over z).
Axes of the slice: x: 2, y: 2, z: 4, core: 2. Of those that a mesh axis runs over, the one named last changes fastest.
Arguments:
- dual_operators: bfloat16 [4, 2, 4, 768, 768], P('gx', 'gy', 'gz'), may hold values from -1 to 3, as said below
- dual_load: float32 [4, 2, 4, 32, 384], P('gx', 'gy', 'gz'), may hold values from -25 to 25
- rigid_modes: float32 [4, 2, 4, 6, 768], P('gx', 'gy', 'gz'), may hold values from -0.21875 to 0.21875
- coarse_load: float32 [4, 2, 4, 6, 32], P('gx', 'gy', 'gz'), may hold values from -24 to 24
- mode_counts: int32 [4, 2, 4], P('gx', 'gy', 'gz'), may hold values from 3 to 6
- face_maps: int32 [4, 2, 4, 3, 128], P('gx', 'gy', 'gz'), may hold values from 0 to 127, each once within a row
Outputs:
- multipliers: float32 [4, 2, 4, 32, 384], P('gx', 'gy', 'gz')
- residual: float32 [4, 2, 4, 32, 384], P('gx', 'gy', 'gz')
The draws below stay inside these ranges and needn't reach their ends.
Inputs may be any that keep to these rules, and one draw needn't show every extreme that they name: Each dual_operators[i, j, k] is symmetric positive definite. Subdomain s uses rows 0 to mode_counts[s] - 1 of rigid_modes[s]. Each face_maps[i, j, k, d] holds every number of 0 to 127 once.
All inputs are finite; a program needn't handle non-finite values.
Results may differ from the reference program's by a relative error of at most 0.012.
Values sent between devices are 32-bit elements; how exact they have to be, the bound alone decides.
A program may use at most 64 MiB of HBM per device.

```python
import math
import jax
import jax.numpy as jnp
from jax import lax

IDOF = 768
FACE = 128
RHS = 32
MODES = 6
ITERS = 2
NSX = 4
NSY = 2
NSZ = 4


def draw_dual_operators(key, part):
    spread = 0.7 / math.sqrt(2.0 * IDOF)
    identity = jnp.eye(IDOF, dtype=jnp.float32)

    def one_column(position):
        column_key = jax.random.fold_in(key, position)
        noise_key = jax.random.fold_in(column_key, 1)
        scale_key = jax.random.fold_in(column_key, 2)
        noise_part = jax.random.truncated_normal(noise_key, -4.0, 4.0, (NSZ, IDOF, IDOF), jnp.float32) * spread
        coupling = identity + 0.5 * (noise_part + jnp.swapaxes(noise_part, 1, 2))
        diagonal = jnp.exp(jax.random.uniform(scale_key, (NSZ, IDOF), jnp.float32, math.log(0.25), math.log(2.0)))
        root_scale = jnp.sqrt(diagonal)
        outer_scale = root_scale[:, :, None] * root_scale[:, None, :]
        return (coupling * outer_scale).astype(jnp.bfloat16)
    blocks = lax.map(one_column, jnp.arange(NSX * NSY))
    return blocks.reshape(NSX, NSY, NSZ, IDOF, IDOF)


def draw_dual_load(key, part):
    grid_key = jax.random.fold_in(key, 11)
    column_key = jax.random.fold_in(key, 12)
    value_key = jax.random.fold_in(key, 13)
    location = (jnp.arange(NSX)[:, None, None] + jnp.arange(NSY)[None, :, None] + jnp.arange(NSZ)[None, None, :]).astype(jnp.float32) / (NSX + NSY + NSZ - 3)
    rising = (1.0 + 2.0 * location) / math.sqrt(3.0)
    subdomain_scale = jnp.exp(jax.random.uniform(grid_key, (NSX, NSY, NSZ), jnp.float32, math.log(0.1), math.log(1.0)))
    column_scale = jnp.exp(jax.random.uniform(column_key, (RHS,), jnp.float32, math.log(0.3), math.log(3.0)))
    full_shape = (NSX, NSY, NSZ, RHS, 3 * FACE)
    values = jax.random.truncated_normal(value_key, -4.0, 4.0, full_shape, jnp.float32)
    scales = (rising * subdomain_scale)[:, :, :, None, None] * column_scale[None, None, None, :, None]
    return values * scales


def set_ends(drawn, own_key, low, high):
    shape = drawn.shape
    index_at = [jax.random.randint(jax.random.fold_in(own_key, axis), (), 0, shape[axis]) for axis in range(len(shape))]
    drawn = drawn.at[tuple(index_at)].set(low)
    longest = shape.index(max(shape))
    index_at[longest] = (index_at[longest] + 1) % shape[longest]
    return drawn.at[tuple(index_at)].set(high)


def shard_levels(own_key, dims, split, smallest, largest):
    gain = 1.0
    for dim, shards_of in split:
        heights = jax.random.uniform(jax.random.fold_in(jax.random.fold_in(own_key, 6), dim), (shards_of,), jnp.float32, smallest / len(split), largest / len(split))
        gain = gain * jnp.repeat(jnp.exp(heights), dims[dim] // shards_of).reshape((-1,) + (1,) * (len(dims) - 1 - dim))
    return gain


def gaussian(own_key, dims, width, bound, cuts=(), kind=jnp.bfloat16):
    loudness = shard_levels(own_key, dims, cuts, -0.22, 0.18) if cuts else 1.0
    array = jax.random.normal(own_key, dims, jnp.float32) * width * loudness
    return jnp.minimum(jnp.maximum(array, -bound), bound).astype(kind)


def setup_inputs(seed: int = 0) -> dict:
    arg_keys = jax.random.split(jax.random.key(seed), 7)
    dual_operators = draw_dual_operators(jax.random.fold_in(arg_keys[6], 71), 0)
    dual_load = draw_dual_load(jax.random.fold_in(arg_keys[6], 71), 0)
    rigid_modes = gaussian(arg_keys[2], (NSX, NSY, NSZ, MODES, IDOF), IDOF ** -0.5, 0.21875, ((0, 4), (1, 2), (2, 4)), jnp.float32)
    coarse_load = gaussian(arg_keys[3], (NSX, NSY, NSZ, MODES, RHS), 4.0, 24.0, ((0, 4), (1, 2), (2, 4)), jnp.float32)
    mode_counts = set_ends(jax.random.randint(arg_keys[4], (NSX, NSY, NSZ), 3, MODES + 1), jax.random.fold_in(arg_keys[4], 1), 3, MODES).astype(jnp.int32)
    face_maps = jax.vmap(lambda own: jax.random.permutation(own, FACE))(jax.random.split(arg_keys[5], NSX * NSY * NSZ * 3)).reshape((NSX, NSY, NSZ, 3, FACE)).astype(jnp.int32)
    return dict(dual_operators=dual_operators, dual_load=dual_load, rigid_modes=rigid_modes, coarse_load=coarse_load, mode_counts=mode_counts, face_maps=face_maps)


def reorder(values, face_order):
    index_table = jnp.broadcast_to(face_order[..., None, :], values.shape)
    return jnp.take_along_axis(values, index_table, axis=-1)

def side_flags(position, extent):
    return jnp.stack([position > 0, position < extent - 1], axis=-1).astype(jnp.float32)

def interface_mask(first_flags, second_flags, third_flags, face_width):
    grid_shape = (first_flags.shape[0], second_flags.shape[0], third_flags.shape[0], 2)
    present = jnp.concatenate([jnp.broadcast_to(first_flags[:, None, None, :], grid_shape), jnp.broadcast_to(second_flags[None, :, None, :], grid_shape), jnp.broadcast_to(third_flags[None, None, :, :], grid_shape)], axis=-1)
    return jnp.repeat(present, face_width, axis=-1)[:, :, :, None, :]

def face_block(values, face_index, face_width):
    return values[..., face_index * face_width:(face_index + 1) * face_width]

def from_lower(block, spatial):
    length = block.shape[spatial]
    padding = jnp.zeros_like(lax.slice_in_dim(block, 0, 1, axis=spatial))
    return jnp.concatenate([padding, lax.slice_in_dim(block, 0, length - 1, axis=spatial)], axis=spatial)

def from_upper(block, spatial):
    length = block.shape[spatial]
    padding = jnp.zeros_like(lax.slice_in_dim(block, 0, 1, axis=spatial))
    return jnp.concatenate([lax.slice_in_dim(block, 1, length, axis=spatial), padding], axis=spatial)

def assemble(local_values, face_maps, inverse, present):
    pieces = []
    for spatial in range(3):
        minus_face = face_block(local_values, 2 * spatial, FACE)
        plus_face = face_block(local_values, 2 * spatial + 1, FACE)
        owner_minus = reorder(minus_face, inverse[:, :, :, spatial, :])
        pieces.append(minus_face - reorder(from_lower(plus_face, spatial), face_maps[:, :, :, spatial, :]))
        pieces.append(plus_face - from_upper(owner_minus, spatial))
    return jnp.concatenate(pieces, axis=-1) * present

def apply_dual(local_values, dual_operators, face_maps, inverse, present):
    rounded = local_values.astype(jnp.bfloat16)

    def one_slab(operands):
        slab_operators, slab_values = operands
        return jnp.einsum('yzrk,yzki->yzri', slab_values.astype(jnp.float32), slab_operators.astype(jnp.float32), precision=lax.Precision.HIGHEST)
    products = lax.map(one_slab, (dual_operators, rounded))
    return assemble(products, face_maps, inverse, present)

def coarse_factor(mode_rows, active):
    identity = jnp.eye(active.shape[-1], dtype=jnp.float32)
    normal_matrix = jnp.einsum('xyzmi,xyzni->xyzmn', mode_rows, mode_rows, precision=lax.Precision.HIGHEST)
    normal_matrix = normal_matrix + identity * (1.0 - active)[..., None, :]
    factor = jnp.linalg.cholesky(normal_matrix)
    return jax.scipy.linalg.cho_solve((factor, True), jnp.broadcast_to(identity, normal_matrix.shape))

def spread_coarse(coefficients, mode_rows):
    return jnp.einsum('xyzmr,xyzmi->xyzri', coefficients, mode_rows, precision=lax.Precision.HIGHEST)

def owned_faces(values):
    return jnp.concatenate([face_block(values, 1, FACE), face_block(values, 3, FACE), face_block(values, 5, FACE)], axis=-1)

def pairing(first_vectors, second_vectors):
    return jnp.einsum('xyzri,xyzsi->rs', owned_faces(first_vectors), owned_faces(second_vectors), precision=lax.Precision.HIGHEST)

def combine_columns(vectors, matrix):
    return jnp.einsum('xyzri,rs->xyzsi', vectors, matrix, precision=lax.Precision.HIGHEST)

def cholesky_solve(matrix, right_side):
    factor = jnp.linalg.cholesky(matrix)
    return jax.scipy.linalg.cho_solve((factor, True), right_side)

def reference(dual_operators, dual_load, rigid_modes, coarse_load, mode_counts, face_maps):
    present = interface_mask(side_flags(jnp.arange(NSX), NSX), side_flags(jnp.arange(NSY), NSY), side_flags(jnp.arange(NSZ), NSZ), FACE)
    inverse = jnp.argsort(face_maps, axis=-1).astype(jnp.int32)
    active = (jnp.arange(MODES)[None, None, None, :] < mode_counts[..., None]).astype(jnp.float32)
    mode_rows = rigid_modes * present * active[..., None]
    coarse_inverse = coarse_factor(mode_rows, active)

    def coarse_field(coefficients):
        return assemble(spread_coarse(coefficients, mode_rows), face_maps, inverse, present)

    def precondition(current):
        weights = jnp.einsum('xyzmi,xyzri->xyzmr', mode_rows, current, precision=lax.Precision.HIGHEST)
        coefficients = jnp.einsum('xyzmn,xyznr->xyzmr', coarse_inverse, weights, precision=lax.Precision.HIGHEST)
        return current - 0.25 * coarse_field(coefficients)

    def operator(current):
        return apply_dual(current, dual_operators, face_maps, inverse, present)
    empty_face = jnp.zeros_like(dual_load[..., :FACE])
    spread_load = jnp.concatenate([empty_face, dual_load[..., :FACE], empty_face, dual_load[..., FACE:2 * FACE], empty_face, dual_load[..., 2 * FACE:]], axis=-1)
    right_local = assemble(spread_load, face_maps, inverse, present)
    initial = coarse_field(jnp.einsum('xyzmn,xyznr->xyzmr', coarse_inverse, coarse_load * active[..., None], precision=lax.Precision.HIGHEST))
    multipliers = initial
    residual = right_local - operator(initial)
    direction = residual
    image = residual
    residual_gram = jnp.zeros((RHS, RHS), jnp.float32)
    for iteration in range(ITERS):
        projected = precondition(residual)
        projected_image = operator(projected)
        fresh_gram = pairing(projected, residual)
        if iteration == 0:
            direction = projected
            image = projected_image
        else:
            update_gram = cholesky_solve(residual_gram, fresh_gram)
            direction = projected + combine_columns(direction, update_gram)
            image = projected_image + combine_columns(image, update_gram)
        residual_gram = fresh_gram
        step_gram = cholesky_solve(pairing(direction, image), residual_gram)
        multipliers = multipliers + combine_columns(direction, step_gram)
        residual = residual - combine_columns(image, step_gram)
    return (owned_faces(multipliers), owned_faces(residual))
```

```python
import functools

import jax
import jax.numpy as jnp
from jax import lax
from jax.experimental import pallas as pl
from jax.experimental.pallas import tpu as pltpu
from jax.sharding import PartitionSpec as P

MESH = pl.DeviceIdType.MESH
HIGH = lax.Precision.HIGHEST
NN = (((1,), (0,)), ((), ()))
NT = (((1,), (1,)), ((), ()))
TN = (((0,), (0,)), ((), ()))


def mul(a, b, dims=NN):
    return lax.dot_general(a, b, dims, precision=HIGH, preferred_element_type=jnp.float32)


def split(a):
    head = a.astype(jnp.bfloat16)
    return head, (a - head.astype(jnp.float32)).astype(jnp.bfloat16)


def fast(a, b, dims=NN):
    if dims == TN:
        a, dims = a.T, NN
    (ah, al), (bh, bl) = split(a), split(b)
    dot = functools.partial(
        lax.dot_general, dimension_numbers=dims, preferred_element_type=jnp.float32
    )
    return dot(ah, bh) + (dot(ah, bl) + dot(al, bh))


def eliminate(system, size, block=8):
    rows = lax.broadcasted_iota(jnp.int32, system.shape, 0)
    span = range(block)
    for k in range(0, size, block):
        columns = [system[:, k + j : k + j + 1] for j in span]
        lines = [system[k + i : k + i + 1, :] for i in span]
        pivots = [
            [jnp.broadcast_to(lines[i][:, k + j : k + j + 1], lines[i].shape) for j in span]
            for i in span
        ]
        for j in span:
            scale = 1.0 / pivots[j][j]
            lines[j] = lines[j] * scale
            pivots[j] = [p * scale for p in pivots[j]]
            for i in span:
                if i != j:
                    factor = pivots[i][j]
                    lines[i] = lines[i] - factor * lines[j]
                    pivots[i] = [p - factor * q for p, q in zip(pivots[i], pivots[j])]
        update = columns[0] * lines[0]
        for j in span[1:]:
            update = update + columns[j] * lines[j]
        system = system - update
        for j in span:
            system = jnp.where(rows == k + j, lines[j], system)
    return system[:, size:]


def identity(size):
    return (
        lax.broadcasted_iota(jnp.int32, (size, size), 0)
        == lax.broadcasted_iota(jnp.int32, (size, size), 1)
    ).astype(jnp.float32)


def packed(gram, width):
    groups = max(1, width // gram.shape[1])
    depth = gram.shape[0] // groups
    return jnp.concatenate([gram[g * depth : (g + 1) * depth] for g in range(groups)], axis=1)


def unpacked(tile, size):
    groups = max(1, tile.shape[1] // size)
    return jnp.concatenate([tile[:, g * size : (g + 1) * size] for g in range(groups)], axis=0)


def kernel(
    extents,
    operator_hbm,
    load_hbm,
    modes_hbm,
    coarse_hbm,
    count_hbm,
    maps_hbm,
    multipliers_ref,
    residual_ref,
    raw,
    load_ref,
    modes_ref,
    coarse_ref,
    maps_ref,
    count_ref,
    ordered,
    own_modes,
    all_modes,
    padded_load,
    probes,
    first_out,
    first_in,
    pair_out,
    pair_in,
    face_out,
    face_in,
    last_out,
    last_in,
    load_in,
    plane_sums,
    line_sums,
    raw_sem,
    first_send,
    first_recv,
    face_send,
    face_recv,
    pair_send,
    pair_recv,
    last_send,
    last_recv,
    load_send,
    load_recv,
    plane_send,
    plane_recv,
    line_send,
    line_recv,
):
    nx, ny, nz = extents
    cases = load_hbm.shape[0]
    width = load_hbm.shape[1] // 3
    modes = modes_hbm.shape[0]
    padded = own_modes.shape[0]
    here = (lax.axis_index("gx"), lax.axis_index("gy"), lax.axis_index("gz"))
    ix, iy, iz = here
    plane = nx * ny
    slot = ix * ny + iy

    fetches = [
        pltpu.make_async_copy(source, target, raw_sem.at[i])
        for i, (source, target) in enumerate(
            (
                (count_hbm, count_ref),
                (maps_hbm, maps_ref),
                (modes_hbm, modes_ref),
                (coarse_hbm, coarse_ref),
                (load_hbm, load_ref),
                (operator_hbm, raw),
            )
        )
    ]
    for fetch in fetches:
        fetch.start()

    def plane_peer(offset):
        other = lax.rem(slot + offset, plane)
        return (lax.div(other, ny), lax.rem(other, ny), iz)

    def line_peers():
        for turn in range(ny):
            for offset in range(1, nz):
                yield (ix, lax.rem(iy + turn, ny), lax.rem(iz + offset, nz))

    exists = []
    neighbour = []
    for d in range(3):
        exists.append(here[d] > 0)
        exists.append(here[d] < extents[d] - 1)
        for step in (-1, 1):
            neighbour.append(tuple(here[a] + (step if a == d else 0) for a in range(3)))
    flags = [jnp.where(e, 1, 0).astype(jnp.int32) for e in exists]

    def moved(position, f):
        return tuple(position[a] + ((2 * (f % 2) - 1) if a == f // 2 else 0) for a in range(3))

    def both_exist(f, g):
        if f != g:
            return jnp.logical_and(exists[f], exists[g])
        if f % 2:
            return here[f // 2] < extents[f // 2] - 2
        return here[f // 2] > 1

    pairs = [
        (f, g)
        for f in range(6)
        for g in range(6)
        if (f == g or f // 2 < g // 2) and extents[f // 2] > 1 + (f == g) and extents[g // 2] > 1
    ]

    first_in[...] = jnp.zeros(first_in.shape, jnp.float32)
    pair_in[...] = jnp.zeros(pair_in.shape, jnp.float32)
    face_in[:, :, cases:, :] = jnp.zeros((2, 6, 2 * padded, width), jnp.float32)

    barrier = pltpu.get_barrier_semaphore()
    diagonal = 0
    for f in range(4):
        for g in range(4, 6):
            peer = moved(moved(here, f), g)

            @pl.when(both_exist(f, g))
            def _(peer=peer):
                pl.semaphore_signal(barrier, inc=1, device_id=peer, device_id_type=MESH)

            diagonal = diagonal + flags[f] * flags[g]
    for offset in range(1, plane):
        pl.semaphore_signal(barrier, inc=1, device_id=plane_peer(offset), device_id_type=MESH)
    for peer in line_peers():
        pl.semaphore_signal(barrier, inc=1, device_id=peer, device_id_type=MESH)

    all_modes[...] = jnp.zeros(all_modes.shape, jnp.float32)
    probes[...] = jnp.zeros(probes.shape, jnp.float32)
    pair_out[...] = jnp.zeros(pair_out.shape, jnp.float32)
    face_out[:, :, cases:, :] = jnp.zeros((2, 6, 2 * padded, width), jnp.float32)
    own_modes[...] = jnp.zeros(own_modes.shape, jnp.float32)
    padded_load[...] = jnp.zeros(padded_load.shape, jnp.float32)

    def face(values, f):
        return values[:, f * width : (f + 1) * width]

    def masked(values, f):
        return jnp.where(jnp.full(values.shape, flags[f], jnp.int32) == 1, values, 0.0)

    sends = [[] for _ in range(6)]
    pair_sends = [[] for _ in pairs]

    def remote(source, target, send, recv, where):
        return pltpu.make_async_remote_copy(
            src_ref=source,
            dst_ref=target,
            send_sem=send,
            recv_sem=recv,
            device_id=where,
            device_id_type=MESH,
        )

    def start_to(f, copies):
        @pl.when(exists[f])
        def _():
            for copy in copies:
                copy.start()

        sends[f].extend(copies)

    for fetch in fetches[:5]:
        fetch.wait()
    def counted(shape):
        return jnp.broadcast_to(count_ref[...], shape)

    lines = lax.broadcasted_iota(jnp.int32, (width, width), 0)
    orders = [(lines == maps_ref[d]).astype(jnp.float32) for d in range(3)]
    for m in range(modes):
        own_modes[m : m + 1, :] = modes_ref[m]
        padded_load[m : m + 1, 0:cases] = coarse_ref[m]
    raw_modes = jnp.where(
        lax.broadcasted_iota(jnp.int32, own_modes.shape, 0) < counted(own_modes.shape), own_modes[...], 0.0
    )
    pieces = []
    for d in range(3):
        pieces.append(masked(mul(face(raw_modes, 2 * d), orders[d], NT), 2 * d))
        pieces.append(masked(face(raw_modes, 2 * d + 1), 2 * d + 1))
    mode_rows = jnp.concatenate(pieces, axis=1)
    own_modes[...] = mode_rows
    all_modes[0:padded, :] = mode_rows
    inactive = lax.broadcasted_iota(jnp.int32, (padded, padded), 0) >= counted((padded, padded))
    normal = mul(mode_rows, mode_rows, NT) + jnp.where(inactive, identity(padded), 0.0)
    coarse_inverse = eliminate(jnp.concatenate([normal, identity(padded)], axis=1), padded)
    active_load = jnp.where(
        lax.broadcasted_iota(jnp.int32, padded_load.shape, 0) < counted(padded_load.shape), padded_load[...], 0.0
    )
    first_part = mul(coarse_inverse, active_load)
    inverse_modes = mul(coarse_inverse, mode_rows)
    probes[6 * padded :, :] = inverse_modes
    for f in range(6):
        first_out[f, 0:padded, :] = -face(mode_rows, f)
        first_out[f, padded : 2 * padded, :] = face(inverse_modes, f)
        first_out[f, 2 * padded :, :] = first_part

    pl.semaphore_wait(barrier, plane - 1 + ny * (nz - 1) + diagonal)

    for f in range(6):
        copies = [
            remote(first_out.at[f], first_in.at[f ^ 1], first_send.at[f], first_recv.at[f ^ 1], neighbour[f])
        ]
        if f % 2:
            d = f // 2
            copies.append(
                remote(
                    load_ref.at[:, pl.ds(d * width, width)],
                    load_in.at[d],
                    load_send.at[d],
                    load_recv.at[d],
                    neighbour[f],
                )
            )
        start_to(f, copies)

    def send_round(phase, values, own=None):
        found = fast(probes[...], values, NT)
        share = found[6 * padded :] if own is None else own - found[6 * padded :]
        for f in range(6):
            face_out[phase, f, 0:cases, :] = face(values, f)
            face_out[phase, f, cases : cases + padded, 0:cases] = share
            face_out[phase, f, cases + padded :, 0:cases] = found[f * padded : (f + 1) * padded]
        for index, (f, g) in enumerate(pairs):
            pair_out[phase, index, 0:padded, 0:cases] = found[f * padded : (f + 1) * padded]
            if f != g:
                pair_out[phase, index, padded:, 0:cases] = found[g * padded : (g + 1) * padded]
        for index, (f, g) in enumerate(pairs):
            other = pairs.index((f ^ 1, g ^ 1))
            copy = remote(
                pair_out.at[phase, index],
                pair_in.at[phase, other],
                pair_send.at[phase, index],
                pair_recv.at[phase, other],
                moved(moved(here, f), g),
            )
            pl.when(both_exist(f, g))(copy.start)
            pair_sends[index].append(copy)
        for f in range(6):
            start_to(
                f,
                [
                    remote(
                        face_out.at[phase, f],
                        face_in.at[phase, f ^ 1],
                        face_send.at[phase, f],
                        face_recv.at[phase, f ^ 1],
                        neighbour[f],
                    )
                ],
            )
        return found, share

    def wait_faces(phase, source, target, send, recv):
        for f in range(6):
            copy = remote(
                source.at[phase, f], target.at[phase, f], send.at[phase, f], recv.at[phase, f], neighbour[f]
            )
            pl.when(exists[f])(copy.wait_recv)

    def wait_pairs(phase):
        for index, (f, g) in enumerate(pairs):
            copy = remote(
                pair_out.at[phase, index],
                pair_in.at[phase, index],
                pair_send.at[phase, index],
                pair_recv.at[phase, index],
                moved(moved(here, f), g),
            )
            pl.when(both_exist(f, g))(copy.wait_recv)

    def assembled(mine, theirs, phase):
        return jnp.concatenate(
            [
                masked(mine[phase, f, 0:cases, :] - theirs[phase, f, 0:cases, :], f)
                for f in range(6)
            ],
            axis=1,
        )

    def apply_local(values):
        head = values.astype(jnp.bfloat16)
        tail = (values - head.astype(jnp.float32)).astype(jnp.bfloat16)
        both = jnp.dot(
            jnp.concatenate([head, tail], axis=0),
            ordered[...],
            preferred_element_type=jnp.float32,
        )
        return both[0:cases] + both[cases:]

    def owned(values):
        return jnp.concatenate([face(values, 1), face(values, 3), face(values, 5)], axis=1)

    fetches[5].wait()
    narrow = [order.astype(jnp.bfloat16) for order in orders]
    for d in range(3):
        low = 2 * d * width
        raw[pl.ds(low, width), :] = jnp.dot(
            narrow[d], raw[pl.ds(low, width), :], preferred_element_type=jnp.float32
        ).astype(jnp.bfloat16)
    for d in range(3):
        low = 2 * d * width
        ordered[:, low : low + width] = lax.dot_general(
            raw[:, low : low + width], narrow[d], NT, preferred_element_type=jnp.float32
        ).astype(jnp.bfloat16)
        ordered[:, low + width : low + 2 * width] = raw[:, low + width : low + 2 * width]
    for f in range(6):
        d = f // 2
        first = remote(first_out.at[f], first_in.at[f], first_send.at[f], first_recv.at[f], neighbour[f])
        pl.when(exists[f])(first.wait_recv)
    coefficients = [first_part]
    for f in range(6):
        all_modes[(1 + f) * padded : (2 + f) * padded, f * width : (f + 1) * width] = first_in[
            f, 0:padded, :
        ]
        probes[f * padded : (f + 1) * padded, f * width : (f + 1) * width] = first_in[
            f, padded : 2 * padded, :
        ]
        coefficients.append(first_in[f, 2 * padded :, :])
    initial = fast(jnp.concatenate(coefficients, axis=0)[:, 0:cases], all_modes[...], TN)
    product = apply_local(initial)
    right = []
    for d in range(3):
        copy = remote(
            load_ref.at[:, pl.ds(d * width, width)],
            load_in.at[d],
            load_send.at[d],
            load_recv.at[d],
            neighbour[2 * d],
        )
        pl.when(exists[2 * d])(copy.wait_recv)
    for d in range(3):
        right.append(masked(-load_in[d], 2 * d))
        right.append(masked(load_ref[:, d * width : (d + 1) * width], 2 * d + 1))
    right = jnp.concatenate(right, axis=1)
    shares = send_round(0, product, fast(inverse_modes, right, NT))
    wait_faces(0, face_out, face_in, face_send, face_recv)
    residual = right - assembled(face_out, face_in, 0)

    def preconditioned(phase, values, shares, sign):
        found, own = shares
        back = face_in[phase, 0, cases + padded :, 0:cases]
        for f in range(1, 6):
            back = back + face_in[phase, f, cases + padded :, 0:cases]
        own = own - sign * back
        wait_pairs(phase)
        terms = [found[f * padded : (f + 1) * padded] for f in range(6)]
        for index, (a, b) in enumerate(pairs):
            terms[b] = terms[b] + pair_in[phase, index, 0:padded, 0:cases]
            if a != b:
                terms[a] = terms[a] + pair_in[phase, index, padded:, 0:cases]
        every = [own]
        for f in range(6):
            every.append(face_in[phase, f, cases : cases + padded, 0:cases] - sign * terms[f])
        return values - 0.25 * fast(jnp.concatenate(every, axis=0), all_modes[...], TN)

    relay = ny - 1
    is_relay = iy == relay

    def gather_copy(which, offset):
        other = lax.rem(ix + offset, nx)
        return remote(
            plane_sums.at[which, slot],
            plane_sums.at[which, slot],
            plane_send.at[which, offset],
            plane_recv.at[which, slot],
            (other, relay, iz),
        )

    def spread_targets():
        for turn in range(ny):
            for offset in range(nz):
                if turn or offset:
                    yield turn * nz + offset, (lax.rem(relay + turn, ny), lax.rem(iz + offset, nz))

    def spread_copy(which, index, position):
        return remote(
            line_sums.at[which, iz],
            line_sums.at[which, iz],
            line_send.at[which, index],
            line_recv.at[which, iz],
            (ix, *position),
        )

    def sum_start(which, tile):
        plane_sums[which, slot] = tile
        for offset in range(nx):
            if offset:
                gather_copy(which, offset).start()
            else:
                pl.when(iy != relay)(gather_copy(which, offset).start)

    def sum_middle(which):
        @pl.when(is_relay)
        def _():
            for other in range(plane):
                copy = remote(
                    plane_sums.at[which, other],
                    plane_sums.at[which, other],
                    plane_send.at[which, 0],
                    plane_recv.at[which, other],
                    (ix, iy, iz),
                )
                pl.when(slot != other)(copy.wait_recv)
            total = plane_sums[which, 0]
            for other in range(1, plane):
                total = total + plane_sums[which, other]
            line_sums[which, iz] = total
            for index, position in spread_targets():
                spread_copy(which, index, position).start()

    def sum_end(which):
        for other in range(nz):
            copy = remote(
                line_sums.at[which, other],
                line_sums.at[which, other],
                line_send.at[which, 0],
                line_recv.at[which, other],
                (ix, iy, iz),
            )
            pl.when(jnp.logical_or(iy != relay, iz != other))(copy.wait_recv)
        total = line_sums[which, 0]
        for other in range(1, nz):
            total = total + line_sums[which, other]
        half = total.shape[0] // 2
        return unpacked(total[0:half], cases), unpacked(total[half:], cases)

    def sum_finish(which):
        for offset in range(nx):
            if offset:
                gather_copy(which, offset).wait_send()
            else:
                pl.when(iy != relay)(gather_copy(which, offset).wait_send)

        @pl.when(is_relay)
        def _():
            for index, position in spread_targets():
                spread_copy(which, index, position).wait_send()

    start = preconditioned(0, residual, shares, -1.0)
    product = apply_local(start)
    shares = send_round(1, product)
    sum_start(
        0,
        jnp.concatenate(
            [
                packed(fast(owned(start), owned(residual), NT), width),
                packed(fast(start, product, NT), width),
            ],
            axis=0,
        ),
    )
    wait_faces(1, face_out, face_in, face_send, face_recv)
    image = assembled(face_out, face_in, 1)
    sum_middle(0)
    second = preconditioned(1, image, shares, 1.0)
    product = apply_local(second)
    sum_start(
        1,
        jnp.concatenate(
            [
                packed(fast(owned(second), owned(image), NT), width),
                packed(fast(second, product, NT), width),
            ],
            axis=0,
        ),
    )
    for f in range(6):
        last_out[0, f] = face(product, f)
    for f in range(6):
        start_to(
            f,
            [
                remote(
                    last_out.at[0, f],
                    last_in.at[0, f ^ 1],
                    last_send.at[0, f],
                    last_recv.at[0, f ^ 1],
                    neighbour[f],
                )
            ],
        )
    sum_middle(1)
    gram, energy = sum_end(0)
    inverse = eliminate(jnp.concatenate([energy, identity(cases)], axis=1), cases)
    alpha = fast(inverse, gram)
    wait_faces(0, last_out, last_in, last_send, last_recv)
    second_image = assembled(last_out, last_in, 0)
    cross, last = sum_end(1)
    carried = fast(inverse, cross)
    schur = last - fast(cross, carried)
    right_side = fast(cross, alpha) - energy
    tail = eliminate(jnp.concatenate([schur, right_side], axis=1), cases)
    head = alpha + fast(carried, tail)
    both = jnp.concatenate([head, -tail], axis=0)
    multipliers_ref[...] = owned(initial) + fast(
        both, jnp.concatenate([owned(start), owned(second)], axis=0), TN
    )
    residual_ref[...] = owned(residual) - fast(
        both, jnp.concatenate([owned(image), owned(second_image)], axis=0), TN
    )

    def finish(condition, copies):
        @pl.when(condition)
        def _():
            for copy in copies:
                copy.wait_send()

    for f in range(6):
        finish(exists[f], sends[f])
    for index, (f, g) in enumerate(pairs):
        finish(both_exist(f, g), pair_sends[index])
    for which in range(2):
        sum_finish(which)


def put_out(multipliers_ref, residual_ref, multipliers_hbm, residual_hbm, sem):
    copies = [
        pltpu.make_async_copy(multipliers_ref, multipliers_hbm, sem.at[0]),
        pltpu.make_async_copy(residual_ref, residual_hbm, sem.at[1]),
    ]
    for copy in copies:
        copy.start()
    for copy in copies:
        copy.wait()


def held(array):
    return pltpu.with_memory_space_constraint(array, pltpu.HBM)


def rows_apart(array):
    return jnp.swapaxes(array, 2, 3).reshape(array.shape[3], 1, array.shape[4])


def local(extents, dual_operators, dual_load, rigid_modes, coarse_load, mode_counts, face_maps):
    size = dual_operators.shape[-1]
    cases = dual_load.shape[-2]
    width = dual_load.shape[-1] // 3
    modes = rigid_modes.shape[-2]
    padded = -(-modes // 8) * 8
    nx, ny, nz = extents
    plane = nx * ny
    tile = 2 * cases // max(1, width // cases)
    f32 = jnp.float32
    vmem = pl.BlockSpec(memory_space=pltpu.VMEM)
    hbm = pl.BlockSpec(memory_space=pltpu.HBM)
    dma = pltpu.SemaphoreType.DMA
    out = jax.ShapeDtypeStruct((cases, 3 * width), f32)
    multipliers, residual = pl.pallas_call(
        functools.partial(kernel, extents),
        out_shape=(out, out),
        in_specs=[
            hbm,
            hbm,
            hbm,
            hbm,
            hbm,
            hbm,
        ],
        out_specs=(vmem, vmem),
        scratch_shapes=[
            pltpu.VMEM((size, size), dual_operators.dtype),
            pltpu.VMEM((cases, 3 * width), f32),
            pltpu.VMEM((modes, 1, size), f32),
            pltpu.VMEM((modes, 1, cases), f32),
            pltpu.VMEM((3, 1, width), jnp.int32),
            pltpu.VMEM((1, 1), jnp.int32),
            pltpu.VMEM((size, size), dual_operators.dtype),
            pltpu.VMEM((padded, size), f32),
            pltpu.VMEM((7 * padded, size), f32),
            pltpu.VMEM((padded, width), f32),
            pltpu.VMEM((7 * padded, size), f32),
            pltpu.VMEM((6, 3 * padded, width), f32),
            pltpu.VMEM((6, 3 * padded, width), f32),
            pltpu.VMEM((2, 18, 2 * padded, width), f32),
            pltpu.VMEM((2, 18, 2 * padded, width), f32),
            pltpu.VMEM((2, 6, cases + 2 * padded, width), f32),
            pltpu.VMEM((2, 6, cases + 2 * padded, width), f32),
            pltpu.VMEM((1, 6, cases, width), f32),
            pltpu.VMEM((1, 6, cases, width), f32),
            pltpu.VMEM((3, cases, width), f32),
            pltpu.VMEM((2, plane, tile, width), f32),
            pltpu.VMEM((2, nz, tile, width), f32),
            dma((6,)),
            dma((6,)),
            dma((6,)),
            dma((2, 6)),
            dma((2, 6)),
            dma((2, 18)),
            dma((2, 18)),
            dma((1, 6)),
            dma((1, 6)),
            dma((3,)),
            dma((3,)),
            dma((2, nx)),
            dma((2, plane)),
            dma((2, ny * nz)),
            dma((2, nz)),
        ],
        compiler_params=pltpu.CompilerParams(collective_id=0, has_side_effects=True, vmem_limit_bytes=16 * 1024 * 1024
        ),
    )(
        held(dual_operators.reshape(size, size)),
        held(dual_load.reshape(cases, 3 * width)),
        held(rows_apart(rigid_modes)),
        held(rows_apart(coarse_load)),
        mode_counts.reshape(1, 1),
        held(rows_apart(face_maps)),
    )
    multipliers, residual = pl.pallas_call(
        put_out,
        out_shape=(out, out),
        in_specs=[vmem, vmem],
        out_specs=(hbm, hbm),
        scratch_shapes=[dma((2,))],
        compiler_params=pltpu.CompilerParams(vmem_limit_bytes=1024 * 1024),
    )(multipliers, residual)
    shape = (1, 1, 1, cases, 3 * width)
    return multipliers.reshape(shape), residual.reshape(shape)


def solution(mesh):
    extents = (mesh.shape["gx"], mesh.shape["gy"], mesh.shape["gz"])
    spec = P("gx", "gy", "gz", None, None)
    return jax.shard_map(
        functools.partial(local, extents),
        mesh=mesh,
        in_specs=(spec, spec, spec, spec, P("gx", "gy", "gz"), spec),
        out_specs=(spec, spec),
        check_vma=False,
    )
```

```python
import functools

import jax
import jax.numpy as jnp
from jax import lax
from jax.experimental import pallas as pl
from jax.experimental.pallas import tpu as pltpu
from jax.sharding import PartitionSpec as P

MESH = pl.DeviceIdType.MESH
NN = (((1,), (0,)), ((), ()))
NT = (((1,), (1,)), ((), ()))
TN = (((0,), (0,)), ((), ()))


def split(a):
    head = a.astype(jnp.bfloat16)
    return head, (a - head.astype(jnp.float32)).astype(jnp.bfloat16)


def fast(a, b, dims=NN):
    if dims == TN:
        a, dims = a.T, NN
    (ah, al), (bh, bl) = split(a), split(b)
    dot = functools.partial(
        lax.dot_general, dimension_numbers=dims, preferred_element_type=jnp.float32
    )
    return dot(ah, bh) + (dot(ah, bl) + dot(al, bh))


def pivoted(entries, lines):
    span = range(len(lines))
    for j in span:
        scale = 1.0 / entries[j][j]
        lines[j] = lines[j] * scale
        scaled = [entries[j][q] * scale if q > j else None for q in span]
        for i in span:
            if i == j:
                continue
            factor = entries[min(i, j)][max(i, j)]
            for q in range(max(i, j + 1), len(lines)):
                entries[i][q] = entries[i][q] - factor * scaled[q]
            lines[i] = lines[i] - factor * lines[j]
        entries[j] = scaled
    return lines


def first_row(values, i):
    return pltpu.roll(values, values.shape[0] - i, 0)[0:1] if i else values[0:1]


def inverted(columns):
    span = range(len(columns))
    shape = (len(columns), 128)
    rows = lax.broadcasted_iota(jnp.int32, shape, 0)
    lanes = lax.broadcasted_iota(jnp.int32, (1, shape[1]), 1)
    wide = [jnp.broadcast_to(column, shape) for column in columns]
    entries = [[first_row(wide[q], i) if q >= i else None for q in span] for i in span]
    lines = pivoted(entries, [(lanes == i).astype(jnp.float32) for i in span])
    merged = jnp.broadcast_to(lines[0], shape)
    for i in span[1:]:
        merged = jnp.where(rows == i, jnp.broadcast_to(lines[i], shape), merged)
    return merged


def eliminate(system, size, block=8):
    width = system.shape[1]
    shape = (block, width)
    rows = lax.broadcasted_iota(jnp.int32, shape, 0)
    panels = [system[p : p + block] for p in range(0, system.shape[0], block)]
    span = range(block)
    for k in range(0, size, block):
        pivot = panels[k // block]
        lines = [first_row(pivot, i) for i in span]
        entries = [
            [jnp.broadcast_to(lines[i][:, k + q : k + q + 1], (1, width)) if q >= i else None for q in span]
            for i in span
        ]
        columns = [
            [jnp.broadcast_to(panel[:, k + q : k + q + 1], shape) for q in span]
            for panel in panels
            if panel is not pivot
        ]
        lines = pivoted(entries, lines)
        lines = [jnp.broadcast_to(line, shape) for line in lines]
        merged = lines[0]
        for j in span[1:]:
            merged = jnp.where(rows == j, lines[j], merged)
        others = iter(columns)
        updated = []
        for panel in panels:
            if panel is pivot:
                updated.append(merged)
                continue
            column = next(others)
            update = column[0] * lines[0]
            for j in span[1:]:
                update = update + column[j] * lines[j]
            updated.append(panel - update)
        panels = updated
    return jnp.concatenate(panels, axis=0)[:, size:]


def identity(size):
    return (
        lax.broadcasted_iota(jnp.int32, (size, size), 0)
        == lax.broadcasted_iota(jnp.int32, (size, size), 1)
    ).astype(jnp.float32)


def packed(gram, width):
    groups = max(1, width // gram.shape[1])
    depth = gram.shape[0] // groups
    return jnp.concatenate([gram[g * depth : (g + 1) * depth] for g in range(groups)], axis=1)


def unpacked(tile, size):
    groups = max(1, tile.shape[1] // size)
    return jnp.concatenate([tile[:, g * size : (g + 1) * size] for g in range(groups)], axis=0)


def terms_of(left, right):
    total = left[:, 0:1] * right[0:1, :]
    for m in range(1, right.shape[0]):
        total = total + left[:, m : m + 1] * right[m : m + 1, :]
    return total


def thrice_rows(a):
    head = a.astype(jnp.bfloat16).astype(jnp.float32)
    return jnp.concatenate([head, head, a - head], axis=0)


def left_of(a):
    return thrice_rows(a).T.astype(jnp.bfloat16)


def right_of(a):
    head, tail = split(a)
    return jnp.concatenate([head, tail, head], axis=0)


def dot(a, b):
    return jnp.dot(a, b, preferred_element_type=jnp.float32)


def kernel(
    extents,
    operator_hbm,
    load_hbm,
    modes_hbm,
    coarse_hbm,
    count_hbm,
    maps_hbm,
    multipliers_ref,
    residual_ref,
    raw,
    load_ref,
    modes_ref,
    coarse_ref,
    maps_ref,
    count_ref,
    ordered,
    own_modes,
    all_modes,
    padded_load,
    probes,
    first_out,
    first_in,
    value_out,
    value_in,
    tile_out,
    tile_in,
    pair_out,
    pair_in,
    load_in,
    plane_sums,
    line_sums,
    raw_sem,
    first_send,
    first_recv,
    value_send,
    value_recv,
    tile_send,
    tile_recv,
    pair_send,
    pair_recv,
    load_send,
    load_recv,
    plane_send,
    plane_recv,
    line_send,
    line_recv,
):
    nx, ny, nz = extents
    cases = load_hbm.shape[0]
    width = load_hbm.shape[1] // 3
    modes = modes_hbm.shape[0]
    padded = own_modes.shape[0]
    here = (lax.axis_index("gx"), lax.axis_index("gy"), lax.axis_index("gz"))
    ix, iy, iz = here
    plane = nx * ny
    slot = ix * ny + iy

    fetches = [
        pltpu.make_async_copy(source, target, raw_sem.at[i])
        for i, (source, target) in enumerate(
            (
                (modes_hbm, modes_ref),
                (count_hbm, count_ref),
                (coarse_hbm, coarse_ref),
                (maps_hbm, maps_ref),
                (load_hbm, load_ref),
                (operator_hbm, raw),
            )
        )
    ]
    for fetch in fetches:
        fetch.start()

    def plane_peer(offset):
        other = lax.rem(slot + offset, plane)
        return (lax.div(other, ny), lax.rem(other, ny), iz)

    def line_peers():
        for turn in range(ny):
            for offset in range(1, nz):
                yield (ix, lax.rem(iy + turn, ny), lax.rem(iz + offset, nz))

    exists = []
    neighbour = []
    for d in range(3):
        exists.append(here[d] > 0)
        exists.append(here[d] < extents[d] - 1)
        for step in (-1, 1):
            neighbour.append(tuple(here[a] + (step if a == d else 0) for a in range(3)))
    flags = [jnp.where(e, 1, 0).astype(jnp.int32) for e in exists]

    def moved(position, f):
        return tuple(position[a] + ((2 * (f % 2) - 1) if a == f // 2 else 0) for a in range(3))

    def both_exist(f, g):
        if f != g:
            return jnp.logical_and(exists[f], exists[g])
        if f % 2:
            return here[f // 2] < extents[f // 2] - 2
        return here[f // 2] > 1

    pairs = [
        (f, g)
        for f in range(6)
        for g in range(6)
        if (f == g or f // 2 < g // 2) and extents[f // 2] > 1 + (f == g) and extents[g // 2] > 1
    ]

    first_in[...] = jnp.zeros(first_in.shape, jnp.float32)
    pair_in[...] = jnp.zeros(pair_in.shape, jnp.float32)
    tile_in[...] = jnp.zeros(tile_in.shape, jnp.float32)

    barrier = pltpu.get_barrier_semaphore()
    def greet(peer):
        pl.semaphore_signal(barrier, inc=1, device_id=peer, device_id_type=MESH)

    expected = 0
    for f in range(6):
        pl.when(exists[f])(functools.partial(greet, neighbour[f]))
        expected = expected + flags[f]
    if max(nx, nz) + ny > 6:
        for f, g in pairs:
            pl.when(both_exist(f, g))(functools.partial(greet, moved(moved(here, f), g)))
            expected = expected + jnp.where(both_exist(f, g), 1, 0).astype(jnp.int32)
        for offset in range(1, plane):
            greet(plane_peer(offset))
        for peer in line_peers():
            greet(peer)
        expected = expected + (plane - 1 + ny * (nz - 1))

    all_modes[...] = jnp.zeros(all_modes.shape, jnp.float32)
    probes[...] = jnp.zeros(probes.shape, jnp.float32)
    own_modes[...] = jnp.zeros(own_modes.shape, jnp.float32)
    padded_load[...] = jnp.zeros(padded_load.shape, jnp.float32)

    def face(values, f):
        return values[:, f * width : (f + 1) * width]

    def masked(values, f):
        return jnp.where(jnp.full(values.shape, flags[f], jnp.int32) == 1, values, 0.0)

    def block(values, f):
        return values[f * padded : (f + 1) * padded]

    def remote(source, target, send, recv, where):
        return pltpu.make_async_remote_copy(
            src_ref=source,
            dst_ref=target,
            send_sem=send,
            recv_sem=recv,
            device_id=where,
            device_id_type=MESH,
        )

    def owned(values):
        return jnp.concatenate([face(values, 1), face(values, 3), face(values, 5)], axis=1)

    sends = []

    def start_if(condition, copy):
        pl.when(condition)(copy.start)
        sends.append((condition, copy))

    for fetch in fetches[:5]:
        fetch.wait()

    def counted(shape):
        return jnp.broadcast_to(count_ref[...], shape)

    lines = lax.broadcasted_iota(jnp.int32, (width, width), 0)
    narrow = [(lines == maps_ref[d]).astype(jnp.float32).astype(jnp.bfloat16) for d in range(3)]
    for m in range(modes):
        own_modes[m : m + 1, :] = modes_ref[m]
        padded_load[m : m + 1, 0:cases] = coarse_ref[m]
    raw_modes = jnp.where(
        lax.broadcasted_iota(jnp.int32, own_modes.shape, 0) < counted(own_modes.shape), own_modes[...], 0.0
    )
    raw_modes = jnp.concatenate([masked(face(raw_modes, f), f) for f in range(6)], axis=1)
    exact = []
    rest = raw_modes
    for _ in range(3):
        exact.append(rest.astype(jnp.bfloat16).astype(jnp.float32))
        rest = rest - exact[-1]
    exact = jnp.concatenate(exact, axis=0).astype(jnp.bfloat16)
    pieces = []
    for d in range(3):
        found = lax.dot_general(face(exact, 2 * d), narrow[d], NT, preferred_element_type=jnp.float32)
        pieces.append(found[0:padded] + found[padded : 2 * padded] + found[2 * padded :])
        pieces.append(face(raw_modes, 2 * d + 1))
    mode_rows = jnp.concatenate(pieces, axis=1)
    mode_index = lax.broadcasted_iota(jnp.int32, (padded, 1), 0)
    inactive = mode_index >= counted((padded, 1))
    columns = []
    for m in range(padded):
        column = jnp.sum(raw_modes * raw_modes[m : m + 1], axis=1, keepdims=True)
        columns.append(column + jnp.where(jnp.logical_and(inactive, mode_index == m), 1.0, 0.0))
    active_load = jnp.where(
        lax.broadcasted_iota(jnp.int32, padded_load.shape, 0) < counted(padded_load.shape), padded_load[...], 0.0
    )
    load_rows = active_load.T[0:cases]
    coarse_inverse = inverted(columns)
    inverse_modes = terms_of(coarse_inverse, mode_rows)
    spread = terms_of(load_rows, inverse_modes)
    for f in range(6):
        value_out[0, f] = face(spread, f)
        first_out[f, 0:padded, :] = -face(mode_rows, f)
        first_out[f, padded:, :] = face(inverse_modes, f)

    pl.semaphore_wait(barrier, expected)

    def value_copy(phase, f, landing):
        return remote(
            value_out.at[phase, f],
            value_in.at[phase, landing],
            value_send.at[phase, f],
            value_recv.at[phase, landing],
            neighbour[f],
        )

    def first_copy(f, landing):
        return remote(first_out.at[f], first_in.at[landing], first_send.at[f], first_recv.at[landing], neighbour[f])

    def load_copy(d, f):
        return remote(
            load_ref.at[:, pl.ds(d * width, width)],
            load_in.at[d],
            load_send.at[d],
            load_recv.at[d],
            neighbour[f],
        )

    def tile_copy(phase, f, landing):
        return remote(
            tile_out.at[phase, f],
            tile_in.at[phase, landing],
            tile_send.at[phase, f],
            tile_recv.at[phase, landing],
            neighbour[f],
        )

    def pair_copy(phase, index, landing):
        f, g = pairs[index]
        return remote(
            pair_out.at[phase, index],
            pair_in.at[phase, landing],
            pair_send.at[phase, index],
            pair_recv.at[phase, landing],
            moved(moved(here, f), g),
        )

    def send_values(phase):
        odd = lax.rem(ix, 2) == 1
        even = jnp.logical_not(odd)
        copies = [value_copy(phase, f, f ^ 1) for f in range(6)]
        start_if(jnp.logical_and(exists[1], odd), copies[1])
        start_if(jnp.logical_and(exists[0], even), copies[0])
        start_if(jnp.logical_and(exists[0], odd), copies[0])
        start_if(jnp.logical_and(exists[1], even), copies[1])
        for f in (4, 5, 2, 3):
            start_if(exists[f], copies[f])

    def wait_values(phase):
        for f in range(6):
            pl.when(exists[f])(value_copy(phase, f, f).wait_recv)

    def send_coefficients(phase, share, found):
        gap = jnp.zeros((padded, width - cases), jnp.float32)
        low = [jnp.concatenate([block(found, f), gap], axis=1) for f in range(6)]
        gap = jnp.zeros((padded, width - 2 * cases), jnp.float32)
        for f in range(6):
            tile_out[phase, f] = jnp.concatenate([share, block(found, f), gap], axis=1)
        for index, (f, g) in enumerate(pairs):
            if f == g:
                pair_out[phase, index] = low[f]
            else:
                pair_out[phase, index] = jnp.concatenate([block(found, f), block(found, g), gap], axis=1)
        def near(index):
            f, g = pairs[index]
            return 2 <= f < 4 or 2 <= g < 4

        def start_pairs(chosen):
            for index in chosen:
                f, g = pairs[index]
                start_if(both_exist(f, g), pair_copy(phase, index, pairs.index((f ^ 1, g ^ 1))))

        start_pairs([index for index in range(len(pairs)) if not near(index)])
        for f in range(6):
            start_if(exists[f], tile_copy(phase, f, f ^ 1))
        start_pairs([index for index in range(len(pairs)) if near(index)])

    def coefficients_of(phase, share, found, sign):
        for f in range(6):
            pl.when(exists[f])(tile_copy(phase, f, f).wait_recv)
        back = tile_in[phase, 0]
        for f in range(1, 6):
            back = back + tile_in[phase, f]
        every = [share - sign * back[:, cases : 2 * cases]]
        for index, (f, g) in enumerate(pairs):
            pl.when(both_exist(f, g))(pair_copy(phase, index, index).wait_recv)
        first = [None] * 6
        second = [None] * 6
        for index, (a, b) in enumerate(pairs):
            tile = pair_in[phase, index]
            first[b] = tile if first[b] is None else first[b] + tile
            if a != b:
                second[a] = tile if second[a] is None else second[a] + tile
        for f in range(6):
            term = block(found, f)
            if first[f] is not None:
                term = term + first[f][:, 0:cases]
            if second[f] is not None:
                term = term + second[f][:, cases : 2 * cases]
            every.append(tile_in[phase, f][:, 0:cases] - sign * term)
        every.append(jnp.zeros((padded, cases), jnp.float32))
        return jnp.concatenate(every, axis=0)

    def assembled(phase):
        return jnp.concatenate(
            [masked(value_out[phase, f] - value_in[phase, f], f) for f in range(6)], axis=1
        )

    def applied(values):
        head, tail = split(values)
        both = dot(jnp.concatenate([head, tail], axis=0), ordered[...])
        half = values.shape[0]
        return both[0:half] + both[half:]

    send_values(0)
    for f in range(6):
        start_if(exists[f], first_copy(f, f ^ 1))
    for d in range(3):
        start_if(exists[2 * d + 1], load_copy(d, 2 * d + 1))

    all_modes[0:padded, :] = mode_rows
    probes[6 * padded : 7 * padded, :] = inverse_modes
    fetches[5].wait()
    for d in range(3):
        low = 2 * d * width
        raw[pl.ds(low, width), :] = dot(narrow[d], raw[pl.ds(low, width), :]).astype(jnp.bfloat16)
    for d in range(3):
        low = 2 * d * width
        ordered[:, low : low + width] = lax.dot_general(
            raw[:, low : low + width], narrow[d], NT, preferred_element_type=jnp.float32
        ).astype(jnp.bfloat16)
        ordered[:, low + width : low + 2 * width] = raw[:, low + width : low + 2 * width]
    wait_values(0)
    for f in range(6):
        pl.when(exists[f])(first_copy(f, f).wait_recv)
    for f in range(6):
        span = slice(f * width, (f + 1) * width)
        all_modes[(1 + f) * padded : (2 + f) * padded, span] = first_in[f, 0:padded, :]
        probes[f * padded : (f + 1) * padded, span] = first_in[f, padded:, :]
    every_probe = split(probes[...])
    initial = assembled(0)
    product = applied(initial)
    for f in range(6):
        value_out[1, f] = face(product, f)
    send_values(1)
    for d in range(3):
        pl.when(exists[2 * d])(load_copy(d, 2 * d).wait_recv)
    right = []
    for d in range(3):
        right.append(masked(-load_in[d], 2 * d))
        right.append(masked(load_ref[:, d * width : (d + 1) * width], 2 * d + 1))
    right = jnp.concatenate(right, axis=1)
    found = fast(probes[...], product, NT)
    shares = fast(inverse_modes, right, NT) - block(found, 6)
    send_coefficients(0, shares, found)
    every_mode = all_modes[...]
    images = applied(jnp.concatenate([every_mode, probes[...]], axis=0))
    depth = every_mode.shape[0]
    probe_image = images[depth:]
    mode_image = images[0:depth]
    cross_image = fast(probe_image, every_mode, NT)
    mode_stack = right_of(every_mode)
    image_stack = right_of(mode_image)
    head, tail = split(cross_image)
    folds = jnp.concatenate([head, head, tail], axis=1)

    def preconditioned(values, image, coefficients):
        left = left_of(0.25 * coefficients)
        return values - dot(left, mode_stack), image - dot(left, image_stack)

    wait_values(1)
    residual = right - assembled(1)
    product = applied(residual)
    probed = fast(probe_image, residual, NT)
    coefficients = coefficients_of(0, shares, found, -1.0)
    start, product = preconditioned(residual, product, coefficients)
    for f in range(6):
        value_out[2, f] = face(product, f)
    send_values(2)
    found = probed - dot(folds, right_of(0.25 * coefficients))
    shares = block(found, 6)
    send_coefficients(1, shares, found)

    relay = ny - 1
    is_relay = iy == relay

    def gather_copy(which, offset):
        other = lax.rem(ix + offset, nx)
        return remote(
            plane_sums.at[which, slot],
            plane_sums.at[which, slot],
            plane_send.at[which, offset],
            plane_recv.at[which, slot],
            (other, relay, iz),
        )

    def spread_targets():
        for turn in range(ny):
            for offset in range(nz):
                if turn or offset:
                    yield turn * nz + offset, (lax.rem(relay + turn, ny), lax.rem(iz + offset, nz))

    def spread_copy(which, index, position):
        return remote(
            line_sums.at[which, iz],
            line_sums.at[which, iz],
            line_send.at[which, index],
            line_recv.at[which, iz],
            (ix, *position),
        )

    def sum_start(which, tile):
        plane_sums[which, slot] = tile
        for offset in range(nx):
            if offset:
                gather_copy(which, offset).start()
            else:
                pl.when(iy != relay)(gather_copy(which, offset).start)

    def sum_middle(which):
        @pl.when(is_relay)
        def _():
            for other in range(plane):
                copy = remote(
                    plane_sums.at[which, other],
                    plane_sums.at[which, other],
                    plane_send.at[which, 0],
                    plane_recv.at[which, other],
                    (ix, iy, iz),
                )
                pl.when(slot != other)(copy.wait_recv)
            total = plane_sums[which, 0]
            for other in range(1, plane):
                total = total + plane_sums[which, other]
            line_sums[which, iz] = total
            for index, position in spread_targets():
                spread_copy(which, index, position).start()

    def sum_end(which):
        for other in range(nz):
            copy = remote(
                line_sums.at[which, other],
                line_sums.at[which, other],
                line_send.at[which, 0],
                line_recv.at[which, other],
                (ix, iy, iz),
            )
            pl.when(jnp.logical_or(iy != relay, iz != other))(copy.wait_recv)
        total = line_sums[which, 0]
        for other in range(1, nz):
            total = total + line_sums[which, other]
        half = total.shape[0] // 2
        return unpacked(total[0:half], cases), unpacked(total[half:], cases)

    def sum_finish(which):
        for offset in range(nx):
            if offset:
                gather_copy(which, offset).wait_send()
            else:
                pl.when(iy != relay)(gather_copy(which, offset).wait_send)

        @pl.when(is_relay)
        def _():
            for index, position in spread_targets():
                spread_copy(which, index, position).wait_send()

    sum_start(
        0,
        jnp.concatenate(
            [
                packed(fast(owned(start), owned(residual), NT), width),
                packed(fast(start, product, NT), width),
            ],
            axis=0,
        ),
    )
    wait_values(2)
    image = assembled(2)
    product = applied(image)
    sum_middle(0)
    coefficients = coefficients_of(1, shares, found, 1.0)
    second, product = preconditioned(image, product, coefficients)
    sum_start(
        1,
        jnp.concatenate(
            [
                packed(fast(owned(second), owned(image), NT), width),
                packed(fast(second, product, NT), width),
            ],
            axis=0,
        ),
    )
    for f in range(6):
        value_out[3, f] = face(product, f)
    send_values(3)
    sum_middle(1)
    gram, energy = sum_end(0)
    inverse = eliminate(jnp.concatenate([energy, identity(cases)], axis=1), cases)
    alpha = fast(inverse, gram)
    starts = jnp.concatenate([owned(start), -owned(image)], axis=1)
    base = jnp.concatenate([owned(initial), owned(residual)], axis=1) + fast(alpha, starts, TN)
    wait_values(3)
    seconds = jnp.concatenate([owned(second), -owned(assembled(3))], axis=1)
    for condition, copy in sends:
        pl.when(condition)(copy.wait_send)
    sum_finish(0)
    cross, last = sum_end(1)
    carried = fast(inverse, cross)
    schur = last - fast(cross, carried)
    right_side = fast(cross, alpha) - energy
    tail = eliminate(jnp.concatenate([schur, right_side], axis=1), cases)
    steps = right_of(seconds - fast(carried, starts, TN))
    result = base - dot(left_of(tail), steps)
    multipliers_ref[...] = result[:, 0 : 3 * width]
    residual_ref[...] = result[:, 3 * width :]
    sum_finish(1)


def put_out(multipliers_ref, residual_ref, multipliers_hbm, residual_hbm, sem):
    copies = [
        pltpu.make_async_copy(multipliers_ref, multipliers_hbm, sem.at[0]),
        pltpu.make_async_copy(residual_ref, residual_hbm, sem.at[1]),
    ]
    for copy in copies:
        copy.start()
    for copy in copies:
        copy.wait()


def held(array):
    return pltpu.with_memory_space_constraint(array, pltpu.HBM)


def rows_apart(array):
    return jnp.swapaxes(array, 2, 3).reshape(array.shape[3], 1, array.shape[4])


def local(extents, dual_operators, dual_load, rigid_modes, coarse_load, mode_counts, face_maps):
    size = dual_operators.shape[-1]
    cases = dual_load.shape[-2]
    width = dual_load.shape[-1] // 3
    modes = rigid_modes.shape[-2]
    padded = -(-modes // 8) * 8
    nx, ny, nz = extents
    plane = nx * ny
    tile = 2 * cases // max(1, width // cases)
    f32 = jnp.float32
    vmem = pl.BlockSpec(memory_space=pltpu.VMEM)
    hbm = pl.BlockSpec(memory_space=pltpu.HBM)
    dma = pltpu.SemaphoreType.DMA
    out = jax.ShapeDtypeStruct((cases, 3 * width), f32)
    multipliers, residual = pl.pallas_call(
        functools.partial(kernel, extents),
        out_shape=(out, out),
        in_specs=[
            hbm,
            hbm,
            hbm,
            hbm,
            hbm,
            hbm,
        ],
        out_specs=(vmem, vmem),
        scratch_shapes=[
            pltpu.VMEM((size, size), dual_operators.dtype),
            pltpu.VMEM((cases, 3 * width), f32),
            pltpu.VMEM((modes, 1, size), f32),
            pltpu.VMEM((modes, 1, cases), f32),
            pltpu.VMEM((3, 1, width), jnp.int32),
            pltpu.VMEM((1, 1), jnp.int32),
            pltpu.VMEM((size, size), dual_operators.dtype),
            pltpu.VMEM((padded, size), f32),
            pltpu.VMEM((8 * padded, size), f32),
            pltpu.VMEM((padded, width), f32),
            pltpu.VMEM((8 * padded, size), f32),
            pltpu.VMEM((6, 2 * padded, width), f32),
            pltpu.VMEM((6, 2 * padded, width), f32),
            pltpu.VMEM((4, 6, cases, width), f32),
            pltpu.VMEM((4, 6, cases, width), f32),
            pltpu.VMEM((2, 6, padded, width), f32),
            pltpu.VMEM((2, 6, padded, width), f32),
            pltpu.VMEM((2, 18, padded, width), f32),
            pltpu.VMEM((2, 18, padded, width), f32),
            pltpu.VMEM((3, cases, width), f32),
            pltpu.VMEM((2, plane, tile, width), f32),
            pltpu.VMEM((2, nz, tile, width), f32),
            dma((6,)),
            dma((6,)),
            dma((6,)),
            dma((4, 6)),
            dma((4, 6)),
            dma((2, 6)),
            dma((2, 6)),
            dma((2, 18)),
            dma((2, 18)),
            dma((3,)),
            dma((3,)),
            dma((2, nx)),
            dma((2, plane)),
            dma((2, ny * nz)),
            dma((2, nz)),
        ],
        compiler_params=pltpu.CompilerParams(collective_id=0, has_side_effects=True, vmem_limit_bytes=16 * 1024 * 1024
        ),
    )(
        held(dual_operators.reshape(size, size)),
        held(dual_load.reshape(cases, 3 * width)),
        held(rows_apart(rigid_modes)),
        held(rows_apart(coarse_load)),
        mode_counts.reshape(1, 1),
        held(rows_apart(face_maps)),
    )
    multipliers, residual = pl.pallas_call(
        put_out,
        out_shape=(out, out),
        in_specs=[vmem, vmem],
        out_specs=(hbm, hbm),
        scratch_shapes=[dma((2,))],
        compiler_params=pltpu.CompilerParams(vmem_limit_bytes=1024 * 1024),
    )(multipliers, residual)
    shape = (1, 1, 1, cases, 3 * width)
    return multipliers.reshape(shape), residual.reshape(shape)


def solution(mesh):
    extents = (mesh.shape["gx"], mesh.shape["gy"], mesh.shape["gz"])
    spec = P("gx", "gy", "gz", None, None)
    return jax.shard_map(
        functools.partial(local, extents),
        mesh=mesh,
        in_specs=(spec, spec, spec, spec, P("gx", "gy", "gz"), spec),
        out_specs=(spec, spec),
        check_vma=False,
    )
```

```python
import functools

import jax
import jax.numpy as jnp
from jax import lax
from jax.experimental import pallas as pl
from jax.experimental.pallas import tpu as pltpu
from jax.sharding import PartitionSpec as P

MESH = pl.DeviceIdType.MESH
NN = (((1,), (0,)), ((), ()))
NT = (((1,), (1,)), ((), ()))
TN = (((0,), (0,)), ((), ()))


def split(a):
    head = a.astype(jnp.bfloat16)
    return head, (a - head.astype(jnp.float32)).astype(jnp.bfloat16)


def fast(a, b, dims=NN):
    if dims == TN:
        a, dims = a.T, NN
    (ah, al), (bh, bl) = split(a), split(b)
    dot = functools.partial(
        lax.dot_general, dimension_numbers=dims, preferred_element_type=jnp.float32
    )
    return dot(ah, bh) + (dot(ah, bl) + dot(al, bh))


def pivoted(entries, lines):
    span = range(len(lines))
    for j in span:
        scale = 1.0 / entries[j][j]
        lines[j] = lines[j] * scale
        scaled = [entries[j][q] * scale if q > j else None for q in span]
        for i in span:
            if i == j:
                continue
            factor = entries[min(i, j)][max(i, j)]
            for q in range(max(i, j + 1), len(lines)):
                entries[i][q] = entries[i][q] - factor * scaled[q]
            lines[i] = lines[i] - factor * lines[j]
        entries[j] = scaled
    return lines


def first_row(values, i):
    return pltpu.roll(values, values.shape[0] - i, 0)[0:1] if i else values[0:1]


def inverted(columns):
    span = range(len(columns))
    shape = (len(columns), 128)
    rows = lax.broadcasted_iota(jnp.int32, shape, 0)
    lanes = lax.broadcasted_iota(jnp.int32, (1, shape[1]), 1)
    wide = [jnp.broadcast_to(column, shape) for column in columns]
    entries = [[first_row(wide[q], i) if q >= i else None for q in span] for i in span]
    lines = pivoted(entries, [(lanes == i).astype(jnp.float32) for i in span])
    merged = jnp.broadcast_to(lines[0], shape)
    for i in span[1:]:
        merged = jnp.where(rows == i, jnp.broadcast_to(lines[i], shape), merged)
    return merged


def eliminate(system, size, block=8):
    width = system.shape[1]
    shape = (block, width)
    rows = lax.broadcasted_iota(jnp.int32, shape, 0)
    panels = [system[p : p + block] for p in range(0, system.shape[0], block)]
    span = range(block)
    for k in range(0, size, block):
        pivot = panels[k // block]
        lines = [first_row(pivot, i) for i in span]
        entries = [
            [jnp.broadcast_to(lines[i][:, k + q : k + q + 1], (1, width)) if q >= i else None for q in span]
            for i in span
        ]
        columns = [
            [jnp.broadcast_to(panel[:, k + q : k + q + 1], shape) for q in span]
            for panel in panels
            if panel is not pivot
        ]
        lines = pivoted(entries, lines)
        lines = [jnp.broadcast_to(line, shape) for line in lines]
        merged = lines[0]
        for j in span[1:]:
            merged = jnp.where(rows == j, lines[j], merged)
        others = iter(columns)
        updated = []
        for panel in panels:
            if panel is pivot:
                updated.append(merged)
                continue
            column = next(others)
            update = column[0] * lines[0]
            for j in span[1:]:
                update = update + column[j] * lines[j]
            updated.append(panel - update)
        panels = updated
    return jnp.concatenate(panels, axis=0)[:, size:]


def identity(size):
    return (
        lax.broadcasted_iota(jnp.int32, (size, size), 0)
        == lax.broadcasted_iota(jnp.int32, (size, size), 1)
    ).astype(jnp.float32)


def packed(gram, width):
    groups = max(1, width // gram.shape[1])
    depth = gram.shape[0] // groups
    return jnp.concatenate([gram[g * depth : (g + 1) * depth] for g in range(groups)], axis=1)


def unpacked(tile, size):
    groups = max(1, tile.shape[1] // size)
    return jnp.concatenate([tile[:, g * size : (g + 1) * size] for g in range(groups)], axis=0)


def terms_of(left, right):
    total = left[:, 0:1] * right[0:1, :]
    for m in range(1, right.shape[0]):
        total = total + left[:, m : m + 1] * right[m : m + 1, :]
    return total


def thrice_rows(a):
    head = a.astype(jnp.bfloat16).astype(jnp.float32)
    return jnp.concatenate([head, head, a - head], axis=0)


def left_of(a):
    return thrice_rows(a).T.astype(jnp.bfloat16)


def right_of(a):
    head, tail = split(a)
    return jnp.concatenate([head, tail, head], axis=0)


def dot(a, b):
    return jnp.dot(a, b, preferred_element_type=jnp.float32)


def kernel(
    extents,
    operator_hbm,
    load_hbm,
    modes_hbm,
    coarse_hbm,
    count_hbm,
    maps_hbm,
    multipliers_ref,
    residual_ref,
    raw,
    load_ref,
    modes_ref,
    coarse_ref,
    maps_ref,
    count_ref,
    ordered,
    own_modes,
    all_modes,
    padded_load,
    probes,
    first_out,
    first_in,
    value_out,
    value_in,
    tile_out,
    tile_in,
    pair_out,
    pair_in,
    load_in,
    plane_sums,
    line_sums,
    raw_sem,
    first_send,
    first_recv,
    value_send,
    value_recv,
    tile_send,
    tile_recv,
    pair_send,
    pair_recv,
    load_send,
    load_recv,
    plane_send,
    plane_recv,
    line_send,
    line_recv,
):
    nx, ny, nz = extents
    cases = load_hbm.shape[0]
    width = load_hbm.shape[1] // 3
    modes = modes_hbm.shape[0]
    padded = own_modes.shape[0]
    here = (lax.axis_index("gx"), lax.axis_index("gy"), lax.axis_index("gz"))
    ix, iy, iz = here
    plane = nx * ny
    slot = ix * ny + iy

    fetches = [
        pltpu.make_async_copy(source, target, raw_sem.at[i])
        for i, (source, target) in enumerate(
            (
                (modes_hbm, modes_ref),
                (count_hbm, count_ref),
                (coarse_hbm, coarse_ref),
                (maps_hbm, maps_ref),
                (load_hbm, load_ref),
                (operator_hbm, raw),
            )
        )
    ]
    for fetch in fetches:
        fetch.start()

    def plane_peer(offset):
        other = lax.rem(slot + offset, plane)
        return (lax.div(other, ny), lax.rem(other, ny), iz)

    def line_peers():
        for turn in range(ny):
            for offset in range(1, nz):
                yield (ix, lax.rem(iy + turn, ny), lax.rem(iz + offset, nz))

    exists = []
    neighbour = []
    for d in range(3):
        exists.append(here[d] > 0)
        exists.append(here[d] < extents[d] - 1)
        for step in (-1, 1):
            neighbour.append(tuple(here[a] + (step if a == d else 0) for a in range(3)))
    flags = [jnp.where(e, 1, 0).astype(jnp.int32) for e in exists]

    def moved(position, f):
        return tuple(position[a] + ((2 * (f % 2) - 1) if a == f // 2 else 0) for a in range(3))

    def both_exist(f, g):
        if f != g:
            return jnp.logical_and(exists[f], exists[g])
        if f % 2:
            return here[f // 2] < extents[f // 2] - 2
        return here[f // 2] > 1

    pairs = [
        (f, g)
        for f in range(6)
        for g in range(6)
        if (f == g or f // 2 < g // 2) and extents[f // 2] > 1 + (f == g) and extents[g // 2] > 1
    ]

    first_in[...] = jnp.zeros(first_in.shape, jnp.float32)
    pair_in[...] = jnp.zeros(pair_in.shape, jnp.float32)
    tile_in[...] = jnp.zeros(tile_in.shape, jnp.float32)

    barrier = pltpu.get_barrier_semaphore()
    def greet(peer):
        pl.semaphore_signal(barrier, inc=1, device_id=peer, device_id_type=MESH)

    expected = 0
    for f in range(6):
        pl.when(exists[f])(functools.partial(greet, neighbour[f]))
        expected = expected + flags[f]
    if max(nx, nz) + ny > 6:
        for f, g in pairs:
            pl.when(both_exist(f, g))(functools.partial(greet, moved(moved(here, f), g)))
            expected = expected + jnp.where(both_exist(f, g), 1, 0).astype(jnp.int32)
        for offset in range(1, plane):
            greet(plane_peer(offset))
        for peer in line_peers():
            greet(peer)
        expected = expected + (plane - 1 + ny * (nz - 1))

    all_modes[...] = jnp.zeros(all_modes.shape, jnp.float32)
    probes[...] = jnp.zeros(probes.shape, jnp.float32)
    own_modes[...] = jnp.zeros(own_modes.shape, jnp.float32)
    padded_load[...] = jnp.zeros(padded_load.shape, jnp.float32)

    def face(values, f):
        return values[:, f * width : (f + 1) * width]

    def masked(values, f):
        return jnp.where(jnp.full(values.shape, flags[f], jnp.int32) == 1, values, 0.0)

    def block(values, f):
        return values[f * padded : (f + 1) * padded]

    def remote(source, target, send, recv, where):
        return pltpu.make_async_remote_copy(
            src_ref=source,
            dst_ref=target,
            send_sem=send,
            recv_sem=recv,
            device_id=where,
            device_id_type=MESH,
        )

    def owned(values):
        return jnp.concatenate([face(values, 1), face(values, 3), face(values, 5)], axis=1)

    sends = []

    def start_if(condition, copy):
        pl.when(condition)(copy.start)
        sends.append((condition, copy))

    for fetch in fetches[:5]:
        fetch.wait()

    def counted(shape):
        return jnp.broadcast_to(count_ref[...], shape)

    lines = lax.broadcasted_iota(jnp.int32, (width, width), 0)
    narrow = [(lines == maps_ref[d]).astype(jnp.float32).astype(jnp.bfloat16) for d in range(3)]
    for m in range(modes):
        own_modes[m : m + 1, :] = modes_ref[m]
        padded_load[m : m + 1, 0:cases] = coarse_ref[m]
    raw_modes = jnp.where(
        lax.broadcasted_iota(jnp.int32, own_modes.shape, 0) < counted(own_modes.shape), own_modes[...], 0.0
    )
    raw_modes = jnp.concatenate([masked(face(raw_modes, f), f) for f in range(6)], axis=1)
    exact = []
    rest = raw_modes
    for _ in range(3):
        exact.append(rest.astype(jnp.bfloat16).astype(jnp.float32))
        rest = rest - exact[-1]
    exact = jnp.concatenate(exact, axis=0).astype(jnp.bfloat16)
    pieces = []
    for d in range(3):
        found = lax.dot_general(face(exact, 2 * d), narrow[d], NT, preferred_element_type=jnp.float32)
        pieces.append(found[0:padded] + found[padded : 2 * padded] + found[2 * padded :])
        pieces.append(face(raw_modes, 2 * d + 1))
    mode_rows = jnp.concatenate(pieces, axis=1)
    mode_index = lax.broadcasted_iota(jnp.int32, (padded, 1), 0)
    inactive = mode_index >= counted((padded, 1))
    columns = []
    for m in range(padded):
        column = jnp.sum(raw_modes * raw_modes[m : m + 1], axis=1, keepdims=True)
        columns.append(column + jnp.where(jnp.logical_and(inactive, mode_index == m), 1.0, 0.0))
    active_load = jnp.where(
        lax.broadcasted_iota(jnp.int32, padded_load.shape, 0) < counted(padded_load.shape), padded_load[...], 0.0
    )
    load_rows = active_load.T[0:cases]
    coarse_inverse = inverted(columns)
    inverse_modes = terms_of(coarse_inverse, mode_rows)
    spread = terms_of(load_rows, inverse_modes)
    for f in range(6):
        value_out[0, f] = face(spread, f)
        first_out[f, 0:padded, :] = -face(mode_rows, f)
        first_out[f, padded:, :] = face(inverse_modes, f)

    pl.semaphore_wait(barrier, expected)

    def value_copy(phase, f, landing):
        return remote(
            value_out.at[phase, f],
            value_in.at[phase, landing],
            value_send.at[phase, f],
            value_recv.at[phase, landing],
            neighbour[f],
        )

    def first_copy(f, landing):
        return remote(first_out.at[f], first_in.at[landing], first_send.at[f], first_recv.at[landing], neighbour[f])

    def load_copy(d, f):
        return remote(
            load_ref.at[:, pl.ds(d * width, width)],
            load_in.at[d],
            load_send.at[d],
            load_recv.at[d],
            neighbour[f],
        )

    def tile_copy(phase, f, landing):
        return remote(
            tile_out.at[phase, f],
            tile_in.at[phase, landing],
            tile_send.at[phase, f],
            tile_recv.at[phase, landing],
            neighbour[f],
        )

    far = [f != g and f < 2 and g >= 4 for f, g in pairs]

    def pair_part(ref, phase, index, wide):
        return ref.at[phase, index] if wide else ref.at[phase, index, pl.ds(0, padded)]

    def pair_copy(phase, index, landing):
        f, g = pairs[index]
        return remote(
            pair_part(pair_out, phase, index, far[index]),
            pair_part(pair_in, phase, landing, far[index]),
            pair_send.at[phase, index],
            pair_recv.at[phase, landing],
            moved(moved(here, f), g),
        )

    def start_pairs(phase, chosen):
        for index in chosen:
            f, g = pairs[index]
            start_if(both_exist(f, g), pair_copy(phase, index, pairs.index((f ^ 1, g ^ 1))))

    def wait_pairs(phase, chosen):
        for index in chosen:
            f, g = pairs[index]
            pl.when(both_exist(f, g))(pair_copy(phase, index, index).wait_recv)

    far_pairs = [index for index in range(len(pairs)) if far[index]]
    near_pairs = [index for index in range(len(pairs)) if not far[index]]

    def send_values(phase):
        odd = lax.rem(ix, 2) == 1
        even = jnp.logical_not(odd)
        copies = [value_copy(phase, f, f ^ 1) for f in range(6)]
        start_if(jnp.logical_and(exists[1], odd), copies[1])
        start_if(jnp.logical_and(exists[0], even), copies[0])
        start_if(jnp.logical_and(exists[0], odd), copies[0])
        start_if(jnp.logical_and(exists[1], even), copies[1])
        for f in (4, 5, 2, 3):
            start_if(exists[f], copies[f])

    def wait_values(phase):
        for f in range(6):
            pl.when(exists[f])(value_copy(phase, f, f).wait_recv)

    def send_far(phase, found):
        for index in far_pairs:
            f, g = pairs[index]
            pair_out[phase, index, 0:padded, 0:cases] = block(found, f)
            pair_out[phase, index, padded:, 0:cases] = block(found, g)
        start_pairs(phase, far_pairs)

    def send_near(phase, share, found):
        gap = jnp.zeros((padded, width - 2 * cases), jnp.float32)
        for f in range(6):
            tile_out[phase, f] = jnp.concatenate([share, block(found, f), gap], axis=1)
        for f in range(6):
            start_if(exists[f], tile_copy(phase, f, f ^ 1))
        for index in near_pairs:
            f, g = pairs[index]
            if f == g:
                pair_out[phase, index, 0:padded, 0:cases] = block(found, f)
            else:
                pair_out[phase, index, 0:padded, :] = jnp.concatenate([block(found, f), block(found, g), gap], axis=1)
        start_pairs(phase, near_pairs)

    def coefficients_of(phase, share, found, sign):
        for f in range(6):
            pl.when(exists[f])(tile_copy(phase, f, f).wait_recv)
        wait_pairs(phase, near_pairs)
        back = tile_in[phase, 0]
        for f in range(1, 6):
            back = back + tile_in[phase, f]
        own = share - sign * back[:, cases : 2 * cases]
        low = [None] * 6
        high = [None] * 6
        for index in near_pairs:
            a, b = pairs[index]
            tile = pair_in[phase, index, 0:padded]
            low[b] = tile if low[b] is None else low[b] + tile
            if a != b:
                high[a] = tile if high[a] is None else high[a] + tile
        terms = []
        for f in range(6):
            term = block(found, f)
            if low[f] is not None:
                term = term + low[f][:, 0:cases]
            if high[f] is not None:
                term = term + high[f][:, cases : 2 * cases]
            terms.append(tile_in[phase, f][:, 0:cases] - sign * term)
        wait_pairs(phase, far_pairs)
        for index in far_pairs:
            a, b = pairs[index]
            terms[b] = terms[b] - sign * pair_in[phase, index, 0:padded, 0:cases]
            terms[a] = terms[a] - sign * pair_in[phase, index, padded:, 0:cases]
        return jnp.concatenate([own, *terms, jnp.zeros((padded, cases), jnp.float32)], axis=0)

    def assembled(phase):
        return jnp.concatenate(
            [masked(value_out[phase, f] - value_in[phase, f], f) for f in range(6)], axis=1
        )

    def applied(values):
        head, tail = split(values)
        both = dot(jnp.concatenate([head, tail], axis=0), ordered[...])
        half = values.shape[0]
        return both[0:half] + both[half:]

    send_values(0)
    for f in range(6):
        start_if(exists[f], first_copy(f, f ^ 1))
    for d in range(3):
        start_if(exists[2 * d + 1], load_copy(d, 2 * d + 1))

    all_modes[0:padded, :] = mode_rows
    probes[6 * padded : 7 * padded, :] = inverse_modes
    fetches[5].wait()
    for d in range(3):
        low = 2 * d * width
        raw[pl.ds(low, width), :] = dot(narrow[d], raw[pl.ds(low, width), :]).astype(jnp.bfloat16)
    for d in range(3):
        low = 2 * d * width
        ordered[:, low : low + width] = lax.dot_general(
            raw[:, low : low + width], narrow[d], NT, preferred_element_type=jnp.float32
        ).astype(jnp.bfloat16)
        ordered[:, low + width : low + 2 * width] = raw[:, low + width : low + 2 * width]
    wait_values(0)
    for f in range(6):
        pl.when(exists[f])(first_copy(f, f).wait_recv)
    for f in range(6):
        span = slice(f * width, (f + 1) * width)
        all_modes[(1 + f) * padded : (2 + f) * padded, span] = first_in[f, 0:padded, :]
        probes[f * padded : (f + 1) * padded, span] = first_in[f, padded:, :]
    every_probe = split(probes[...])
    initial = assembled(0)
    product = applied(initial)
    for f in range(6):
        value_out[1, f] = face(product, f)
    send_values(1)
    for d in range(3):
        pl.when(exists[2 * d])(load_copy(d, 2 * d).wait_recv)
    right = []
    for d in range(3):
        right.append(masked(-load_in[d], 2 * d))
        right.append(masked(load_ref[:, d * width : (d + 1) * width], 2 * d + 1))
    right = jnp.concatenate(right, axis=1)
    found = fast(probes[...], product, NT)
    shares = fast(inverse_modes, right, NT) - block(found, 6)
    send_far(0, found)
    send_near(0, shares, found)
    every_mode = all_modes[...]
    images = applied(jnp.concatenate([every_mode, probes[...]], axis=0))
    depth = every_mode.shape[0]
    probe_image = images[depth:]
    mode_image = images[0:depth]
    cross_image = fast(probe_image, every_mode, NT)
    mode_stack = right_of(every_mode)
    image_stack = right_of(mode_image)
    head, tail = split(cross_image)
    folds = jnp.concatenate([head, head, tail], axis=1)

    def preconditioned(values, image, coefficients):
        left = left_of(0.25 * coefficients)
        return values - dot(left, mode_stack), image - dot(left, image_stack)

    wait_values(1)
    residual = right - assembled(1)
    product = applied(residual)
    probed = fast(probe_image, residual, NT)
    coefficients = coefficients_of(0, shares, found, -1.0)
    found = probed - dot(folds, right_of(0.25 * coefficients))
    send_far(1, found)
    start, product = preconditioned(residual, product, coefficients)
    for f in range(6):
        value_out[2, f] = face(product, f)
    send_values(2)
    shares = block(found, 6)
    send_near(1, shares, found)

    relay = ny - 1
    is_relay = iy == relay

    def gather_copy(which, offset):
        other = lax.rem(ix + offset, nx)
        return remote(
            plane_sums.at[which, slot],
            plane_sums.at[which, slot],
            plane_send.at[which, offset],
            plane_recv.at[which, slot],
            (other, relay, iz),
        )

    def spread_targets():
        for turn in range(ny):
            for offset in range(nz):
                if turn or offset:
                    yield turn * nz + offset, (lax.rem(relay + turn, ny), lax.rem(iz + offset, nz))

    def spread_copy(which, index, position):
        return remote(
            line_sums.at[which, iz],
            line_sums.at[which, iz],
            line_send.at[which, index],
            line_recv.at[which, iz],
            (ix, *position),
        )

    def sum_start(which, tile):
        plane_sums[which, slot] = tile
        for offset in range(nx):
            if offset:
                gather_copy(which, offset).start()
            else:
                pl.when(iy != relay)(gather_copy(which, offset).start)

    def sum_middle(which):
        @pl.when(is_relay)
        def _():
            for other in range(plane):
                copy = remote(
                    plane_sums.at[which, other],
                    plane_sums.at[which, other],
                    plane_send.at[which, 0],
                    plane_recv.at[which, other],
                    (ix, iy, iz),
                )
                pl.when(slot != other)(copy.wait_recv)
            total = plane_sums[which, 0]
            for other in range(1, plane):
                total = total + plane_sums[which, other]
            line_sums[which, iz] = total
            for index, position in spread_targets():
                spread_copy(which, index, position).start()

    def sum_end(which):
        for other in range(nz):
            copy = remote(
                line_sums.at[which, other],
                line_sums.at[which, other],
                line_send.at[which, 0],
                line_recv.at[which, other],
                (ix, iy, iz),
            )
            pl.when(jnp.logical_or(iy != relay, iz != other))(copy.wait_recv)
        total = line_sums[which, 0]
        for other in range(1, nz):
            total = total + line_sums[which, other]
        half = total.shape[0] // 2
        return unpacked(total[0:half], cases), unpacked(total[half:], cases)

    def sum_finish(which):
        for offset in range(nx):
            if offset:
                gather_copy(which, offset).wait_send()
            else:
                pl.when(iy != relay)(gather_copy(which, offset).wait_send)

        @pl.when(is_relay)
        def _():
            for index, position in spread_targets():
                spread_copy(which, index, position).wait_send()

    sum_start(
        0,
        jnp.concatenate(
            [
                packed(fast(owned(start), owned(residual), NT), width),
                packed(fast(start, product, NT), width),
            ],
            axis=0,
        ),
    )
    wait_values(2)
    image = assembled(2)
    product = applied(image)
    coefficients = coefficients_of(1, shares, found, 1.0)
    second, product = preconditioned(image, product, coefficients)
    sum_start(
        1,
        jnp.concatenate(
            [
                packed(fast(owned(second), owned(image), NT), width),
                packed(fast(second, product, NT), width),
            ],
            axis=0,
        ),
    )
    sum_middle(0)
    for f in range(6):
        value_out[3, f] = face(product, f)
    send_values(3)
    sum_middle(1)
    gram, energy = sum_end(0)
    inverse = eliminate(jnp.concatenate([energy, identity(cases)], axis=1), cases)
    alpha = fast(inverse, gram)
    starts = jnp.concatenate([owned(start), -owned(image)], axis=1)
    base = jnp.concatenate([owned(initial), owned(residual)], axis=1) + fast(alpha, starts, TN)
    wait_values(3)
    seconds = jnp.concatenate([owned(second), -owned(assembled(3))], axis=1)
    for condition, copy in sends:
        pl.when(condition)(copy.wait_send)
    sum_finish(0)
    cross, last = sum_end(1)
    carried = fast(inverse, cross)
    schur = last - fast(cross, carried)
    right_side = fast(cross, alpha) - energy
    tail = eliminate(jnp.concatenate([schur, right_side], axis=1), cases)
    steps = right_of(seconds - fast(carried, starts, TN))
    result = base - dot(left_of(tail), steps)
    multipliers_ref[...] = result[:, 0 : 3 * width]
    residual_ref[...] = result[:, 3 * width :]
    sum_finish(1)


def put_out(multipliers_ref, residual_ref, multipliers_hbm, residual_hbm, sem):
    copies = [
        pltpu.make_async_copy(multipliers_ref, multipliers_hbm, sem.at[0]),
        pltpu.make_async_copy(residual_ref, residual_hbm, sem.at[1]),
    ]
    for copy in copies:
        copy.start()
    for copy in copies:
        copy.wait()


def held(array):
    return pltpu.with_memory_space_constraint(array, pltpu.HBM)


def rows_apart(array):
    return jnp.swapaxes(array, 2, 3).reshape(array.shape[3], 1, array.shape[4])


def local(extents, dual_operators, dual_load, rigid_modes, coarse_load, mode_counts, face_maps):
    size = dual_operators.shape[-1]
    cases = dual_load.shape[-2]
    width = dual_load.shape[-1] // 3
    modes = rigid_modes.shape[-2]
    padded = -(-modes // 8) * 8
    nx, ny, nz = extents
    plane = nx * ny
    tile = 2 * cases // max(1, width // cases)
    f32 = jnp.float32
    vmem = pl.BlockSpec(memory_space=pltpu.VMEM)
    hbm = pl.BlockSpec(memory_space=pltpu.HBM)
    dma = pltpu.SemaphoreType.DMA
    out = jax.ShapeDtypeStruct((cases, 3 * width), f32)
    multipliers, residual = pl.pallas_call(
        functools.partial(kernel, extents),
        out_shape=(out, out),
        in_specs=[
            hbm,
            hbm,
            hbm,
            hbm,
            hbm,
            hbm,
        ],
        out_specs=(vmem, vmem),
        scratch_shapes=[
            pltpu.VMEM((size, size), dual_operators.dtype),
            pltpu.VMEM((cases, 3 * width), f32),
            pltpu.VMEM((modes, 1, size), f32),
            pltpu.VMEM((modes, 1, cases), f32),
            pltpu.VMEM((3, 1, width), jnp.int32),
            pltpu.VMEM((1, 1), jnp.int32),
            pltpu.VMEM((size, size), dual_operators.dtype),
            pltpu.VMEM((padded, size), f32),
            pltpu.VMEM((8 * padded, size), f32),
            pltpu.VMEM((padded, width), f32),
            pltpu.VMEM((8 * padded, size), f32),
            pltpu.VMEM((6, 2 * padded, width), f32),
            pltpu.VMEM((6, 2 * padded, width), f32),
            pltpu.VMEM((4, 6, cases, width), f32),
            pltpu.VMEM((4, 6, cases, width), f32),
            pltpu.VMEM((2, 6, padded, width), f32),
            pltpu.VMEM((2, 6, padded, width), f32),
            pltpu.VMEM((2, 18, 2 * padded, width), f32),
            pltpu.VMEM((2, 18, 2 * padded, width), f32),
            pltpu.VMEM((3, cases, width), f32),
            pltpu.VMEM((2, plane, tile, width), f32),
            pltpu.VMEM((2, nz, tile, width), f32),
            dma((6,)),
            dma((6,)),
            dma((6,)),
            dma((4, 6)),
            dma((4, 6)),
            dma((2, 6)),
            dma((2, 6)),
            dma((2, 18)),
            dma((2, 18)),
            dma((3,)),
            dma((3,)),
            dma((2, nx)),
            dma((2, plane)),
            dma((2, ny * nz)),
            dma((2, nz)),
        ],
        compiler_params=pltpu.CompilerParams(collective_id=0, has_side_effects=True, vmem_limit_bytes=16 * 1024 * 1024
        ),
    )(
        held(dual_operators.reshape(size, size)),
        held(dual_load.reshape(cases, 3 * width)),
        held(rows_apart(rigid_modes)),
        held(rows_apart(coarse_load)),
        mode_counts.reshape(1, 1),
        held(rows_apart(face_maps)),
    )
    multipliers, residual = pl.pallas_call(
        put_out,
        out_shape=(out, out),
        in_specs=[vmem, vmem],
        out_specs=(hbm, hbm),
        scratch_shapes=[dma((2,))],
        compiler_params=pltpu.CompilerParams(vmem_limit_bytes=1024 * 1024),
    )(multipliers, residual)
    shape = (1, 1, 1, cases, 3 * width)
    return multipliers.reshape(shape), residual.reshape(shape)


def solution(mesh):
    extents = (mesh.shape["gx"], mesh.shape["gy"], mesh.shape["gz"])
    spec = P("gx", "gy", "gz", None, None)
    return jax.shard_map(
        functools.partial(local, extents),
        mesh=mesh,
        in_specs=(spec, spec, spec, spec, P("gx", "gy", "gz"), spec),
        out_specs=(spec, spec),
        check_vma=False,
    )
```

```python
import functools

import jax
import jax.numpy as jnp
from jax import lax
from jax.experimental import pallas as pl
from jax.experimental.pallas import tpu as pltpu
from jax.sharding import PartitionSpec as P

MESH = pl.DeviceIdType.MESH
NN = (((1,), (0,)), ((), ()))
NT = (((1,), (1,)), ((), ()))
TN = (((0,), (0,)), ((), ()))


def split(a):
    head = a.astype(jnp.bfloat16)
    return head, (a - head.astype(jnp.float32)).astype(jnp.bfloat16)


def fast(a, b, dims=NN):
    if dims == TN:
        a, dims = a.T, NN
    (ah, al), (bh, bl) = split(a), split(b)
    dot = functools.partial(
        lax.dot_general, dimension_numbers=dims, preferred_element_type=jnp.float32
    )
    return dot(ah, bh) + (dot(ah, bl) + dot(al, bh))


def pivoted(entries, lines):
    span = range(len(lines))
    for j in span:
        scale = 1.0 / entries[j][j]
        lines[j] = lines[j] * scale
        scaled = [entries[j][q] * scale if q > j else None for q in span]
        for i in span:
            if i == j:
                continue
            factor = entries[min(i, j)][max(i, j)]
            for q in range(max(i, j + 1), len(lines)):
                entries[i][q] = entries[i][q] - factor * scaled[q]
            lines[i] = lines[i] - factor * lines[j]
        entries[j] = scaled
    return lines


def first_row(values, i):
    return pltpu.roll(values, values.shape[0] - i, 0)[0:1] if i else values[0:1]


def inverted(columns):
    span = range(len(columns))
    shape = (len(columns), 128)
    rows = lax.broadcasted_iota(jnp.int32, shape, 0)
    lanes = lax.broadcasted_iota(jnp.int32, (1, shape[1]), 1)
    wide = [jnp.broadcast_to(column, shape) for column in columns]
    entries = [[first_row(wide[q], i) if q >= i else None for q in span] for i in span]
    lines = pivoted(entries, [(lanes == i).astype(jnp.float32) for i in span])
    merged = jnp.broadcast_to(lines[0], shape)
    for i in span[1:]:
        merged = jnp.where(rows == i, jnp.broadcast_to(lines[i], shape), merged)
    return merged


def eliminate(system, size, block=8):
    width = system.shape[1]
    shape = (block, width)
    rows = lax.broadcasted_iota(jnp.int32, shape, 0)
    panels = [system[p : p + block] for p in range(0, system.shape[0], block)]
    span = range(block)
    for k in range(0, size, block):
        pivot = panels[k // block]
        lines = [first_row(pivot, i) for i in span]
        entries = [
            [jnp.broadcast_to(lines[i][:, k + q : k + q + 1], (1, width)) if q >= i else None for q in span]
            for i in span
        ]
        columns = [
            [jnp.broadcast_to(panel[:, k + q : k + q + 1], shape) for q in span]
            for panel in panels
            if panel is not pivot
        ]
        lines = pivoted(entries, lines)
        lines = [jnp.broadcast_to(line, shape) for line in lines]
        merged = lines[0]
        for j in span[1:]:
            merged = jnp.where(rows == j, lines[j], merged)
        others = iter(columns)
        updated = []
        for panel in panels:
            if panel is pivot:
                updated.append(merged)
                continue
            column = next(others)
            update = column[0] * lines[0]
            for j in span[1:]:
                update = update + column[j] * lines[j]
            updated.append(panel - update)
        panels = updated
    return jnp.concatenate(panels, axis=0)[:, size:]


def identity(size):
    return (
        lax.broadcasted_iota(jnp.int32, (size, size), 0)
        == lax.broadcasted_iota(jnp.int32, (size, size), 1)
    ).astype(jnp.float32)


def packed(gram, width):
    groups = max(1, width // gram.shape[1])
    depth = gram.shape[0] // groups
    return jnp.concatenate([gram[g * depth : (g + 1) * depth] for g in range(groups)], axis=1)


def unpacked(tile, size):
    groups = max(1, tile.shape[1] // size)
    return jnp.concatenate([tile[:, g * size : (g + 1) * size] for g in range(groups)], axis=0)


def terms_of(left, right):
    total = left[:, 0:1] * right[0:1, :]
    for m in range(1, right.shape[0]):
        total = total + left[:, m : m + 1] * right[m : m + 1, :]
    return total


def thrice_rows(a):
    head = a.astype(jnp.bfloat16).astype(jnp.float32)
    return jnp.concatenate([head, head, a - head], axis=0)


def left_of(a):
    return thrice_rows(a).T.astype(jnp.bfloat16)


def right_of(a):
    head, tail = split(a)
    return jnp.concatenate([head, tail, head], axis=0)


def dot(a, b):
    return jnp.dot(a, b, preferred_element_type=jnp.float32)


def kernel(
    extents,
    operator_hbm,
    load_hbm,
    modes_hbm,
    coarse_hbm,
    count_hbm,
    maps_hbm,
    multipliers_ref,
    residual_ref,
    raw,
    load_ref,
    modes_ref,
    coarse_ref,
    maps_ref,
    count_ref,
    ordered,
    own_modes,
    all_modes,
    padded_load,
    probes,
    first_out,
    first_in,
    value_out,
    value_in,
    tile_out,
    tile_in,
    pair_out,
    pair_in,
    load_in,
    plane_sums,
    line_sums,
    raw_sem,
    first_send,
    first_recv,
    value_send,
    value_recv,
    tile_send,
    tile_recv,
    pair_send,
    pair_recv,
    load_send,
    load_recv,
    plane_send,
    plane_recv,
    line_send,
    line_recv,
):
    nx, ny, nz = extents
    cases = load_hbm.shape[0]
    width = load_hbm.shape[1] // 3
    modes = modes_hbm.shape[0]
    padded = own_modes.shape[0]
    here = (lax.axis_index("gx"), lax.axis_index("gy"), lax.axis_index("gz"))
    ix, iy, iz = here
    plane = nx * ny
    slot = ix * ny + iy

    fetches = [
        pltpu.make_async_copy(source, target, raw_sem.at[i])
        for i, (source, target) in enumerate(
            (
                (modes_hbm, modes_ref),
                (count_hbm, count_ref),
                (coarse_hbm, coarse_ref),
                (maps_hbm, maps_ref),
                (load_hbm, load_ref),
                (operator_hbm, raw),
            )
        )
    ]
    for fetch in fetches:
        fetch.start()

    def plane_peer(offset):
        other = lax.rem(slot + offset, plane)
        return (lax.div(other, ny), lax.rem(other, ny), iz)

    def line_peers():
        for turn in range(ny):
            for offset in range(1, nz):
                yield (ix, lax.rem(iy + turn, ny), lax.rem(iz + offset, nz))

    exists = []
    neighbour = []
    for d in range(3):
        exists.append(here[d] > 0)
        exists.append(here[d] < extents[d] - 1)
        for step in (-1, 1):
            neighbour.append(tuple(here[a] + (step if a == d else 0) for a in range(3)))
    flags = [jnp.where(e, 1, 0).astype(jnp.int32) for e in exists]

    def moved(position, f):
        return tuple(position[a] + ((2 * (f % 2) - 1) if a == f // 2 else 0) for a in range(3))

    def both_exist(f, g):
        if f != g:
            return jnp.logical_and(exists[f], exists[g])
        if f % 2:
            return here[f // 2] < extents[f // 2] - 2
        return here[f // 2] > 1

    pairs = [
        (f, g)
        for f in range(6)
        for g in range(6)
        if (f == g or f // 2 < g // 2) and extents[f // 2] > 1 + (f == g) and extents[g // 2] > 1
    ]

    first_in[...] = jnp.zeros(first_in.shape, jnp.float32)
    pair_in[...] = jnp.zeros(pair_in.shape, jnp.float32)
    tile_in[...] = jnp.zeros(tile_in.shape, jnp.float32)

    barrier = pltpu.get_barrier_semaphore()
    def greet(peer):
        pl.semaphore_signal(barrier, inc=1, device_id=peer, device_id_type=MESH)

    expected = 0
    for f in range(6):
        pl.when(exists[f])(functools.partial(greet, neighbour[f]))
        expected = expected + flags[f]
    if max(nx, nz) + ny > 6:
        for f, g in pairs:
            pl.when(both_exist(f, g))(functools.partial(greet, moved(moved(here, f), g)))
            expected = expected + jnp.where(both_exist(f, g), 1, 0).astype(jnp.int32)
        for offset in range(1, plane):
            greet(plane_peer(offset))
        for peer in line_peers():
            greet(peer)
        expected = expected + (plane - 1 + ny * (nz - 1))

    all_modes[...] = jnp.zeros(all_modes.shape, jnp.float32)
    probes[...] = jnp.zeros(probes.shape, jnp.float32)
    own_modes[...] = jnp.zeros(own_modes.shape, jnp.float32)
    padded_load[...] = jnp.zeros(padded_load.shape, jnp.float32)

    def face(values, f):
        return values[:, f * width : (f + 1) * width]

    def masked(values, f):
        return jnp.where(jnp.full(values.shape, flags[f], jnp.int32) == 1, values, 0.0)

    def block(values, f):
        return values[f * padded : (f + 1) * padded]

    def remote(source, target, send, recv, where):
        return pltpu.make_async_remote_copy(
            src_ref=source,
            dst_ref=target,
            send_sem=send,
            recv_sem=recv,
            device_id=where,
            device_id_type=MESH,
        )

    def owned(values):
        return jnp.concatenate([face(values, 1), face(values, 3), face(values, 5)], axis=1)

    sends = []

    def start_if(condition, copy):
        pl.when(condition)(copy.start)
        sends.append((condition, copy))

    for fetch in fetches[:5]:
        fetch.wait()

    def counted(shape):
        return jnp.broadcast_to(count_ref[...], shape)

    lines = lax.broadcasted_iota(jnp.int32, (width, width), 0)
    narrow = [(lines == maps_ref[d]).astype(jnp.float32).astype(jnp.bfloat16) for d in range(3)]
    for m in range(modes):
        own_modes[m : m + 1, :] = modes_ref[m]
        padded_load[m : m + 1, 0:cases] = coarse_ref[m]
    raw_modes = jnp.where(
        lax.broadcasted_iota(jnp.int32, own_modes.shape, 0) < counted(own_modes.shape), own_modes[...], 0.0
    )
    raw_modes = jnp.concatenate([masked(face(raw_modes, f), f) for f in range(6)], axis=1)
    exact = []
    rest = raw_modes
    for _ in range(3):
        exact.append(rest.astype(jnp.bfloat16).astype(jnp.float32))
        rest = rest - exact[-1]
    exact = jnp.concatenate(exact, axis=0).astype(jnp.bfloat16)
    pieces = []
    for d in range(3):
        found = lax.dot_general(face(exact, 2 * d), narrow[d], NT, preferred_element_type=jnp.float32)
        pieces.append(found[0:padded] + found[padded : 2 * padded] + found[2 * padded :])
        pieces.append(face(raw_modes, 2 * d + 1))
    mode_rows = jnp.concatenate(pieces, axis=1)
    mode_index = lax.broadcasted_iota(jnp.int32, (padded, 1), 0)
    inactive = mode_index >= counted((padded, 1))
    columns = []
    for m in range(padded):
        column = jnp.sum(raw_modes * raw_modes[m : m + 1], axis=1, keepdims=True)
        columns.append(column + jnp.where(jnp.logical_and(inactive, mode_index == m), 1.0, 0.0))
    active_load = jnp.where(
        lax.broadcasted_iota(jnp.int32, padded_load.shape, 0) < counted(padded_load.shape), padded_load[...], 0.0
    )
    load_rows = active_load.T[0:cases]
    coarse_inverse = inverted(columns)
    inverse_modes = terms_of(coarse_inverse, mode_rows)
    spread = terms_of(load_rows, inverse_modes)
    for f in range(6):
        value_out[0, f] = face(spread, f)
        first_out[f, 0:padded, :] = -face(mode_rows, f)
        first_out[f, padded:, :] = face(inverse_modes, f)

    pl.semaphore_wait(barrier, expected)

    def value_copy(phase, f, landing):
        return remote(
            value_out.at[phase, f],
            value_in.at[phase, landing],
            value_send.at[phase, f],
            value_recv.at[phase, landing],
            neighbour[f],
        )

    def first_copy(f, landing):
        return remote(first_out.at[f], first_in.at[landing], first_send.at[f], first_recv.at[landing], neighbour[f])

    def load_copy(d, f):
        return remote(
            load_ref.at[:, pl.ds(d * width, width)],
            load_in.at[d],
            load_send.at[d],
            load_recv.at[d],
            neighbour[f],
        )

    def tile_copy(phase, f, landing):
        return remote(
            tile_out.at[phase, f],
            tile_in.at[phase, landing],
            tile_send.at[phase, f],
            tile_recv.at[phase, landing],
            neighbour[f],
        )

    far = [f != g and f < 2 and g >= 4 for f, g in pairs]

    def pair_part(ref, phase, index, wide):
        return ref.at[phase, index] if wide else ref.at[phase, index, pl.ds(0, padded)]

    def pair_copy(phase, index, landing):
        f, g = pairs[index]
        return remote(
            pair_part(pair_out, phase, index, far[index]),
            pair_part(pair_in, phase, landing, far[index]),
            pair_send.at[phase, index],
            pair_recv.at[phase, landing],
            moved(moved(here, f), g),
        )

    def start_pairs(phase, chosen):
        for index in chosen:
            f, g = pairs[index]
            start_if(both_exist(f, g), pair_copy(phase, index, pairs.index((f ^ 1, g ^ 1))))

    def wait_pairs(phase, chosen):
        for index in chosen:
            f, g = pairs[index]
            pl.when(both_exist(f, g))(pair_copy(phase, index, index).wait_recv)

    far_pairs = [index for index in range(len(pairs)) if far[index]]
    near_pairs = [index for index in range(len(pairs)) if not far[index]]

    def send_lines(phase):
        odd = lax.rem(ix, 2) == 1
        even = jnp.logical_not(odd)
        for f, turn in ((1, odd), (0, even), (0, odd), (1, even)):
            start_if(jnp.logical_and(exists[f], turn), value_copy(phase, f, f ^ 1))

    def send_others(phase):
        for f in (4, 5, 2, 3):
            start_if(exists[f], value_copy(phase, f, f ^ 1))

    def send_values(phase):
        send_lines(phase)
        send_others(phase)

    def wait_values(phase):
        for f in range(6):
            pl.when(exists[f])(value_copy(phase, f, f).wait_recv)

    def send_far(phase, found):
        for index in far_pairs:
            f, g = pairs[index]
            pair_out[phase, index, 0:padded, 0:cases] = block(found, f)
            pair_out[phase, index, padded:, 0:cases] = block(found, g)
        start_pairs(phase, far_pairs)

    def send_near(phase, share, found):
        gap = jnp.zeros((padded, width - 2 * cases), jnp.float32)
        for f in range(6):
            tile_out[phase, f] = jnp.concatenate([share, block(found, f), gap], axis=1)
        for f in range(6):
            start_if(exists[f], tile_copy(phase, f, f ^ 1))
        for index in near_pairs:
            f, g = pairs[index]
            if f == g:
                pair_out[phase, index, 0:padded, 0:cases] = block(found, f)
            else:
                pair_out[phase, index, 0:padded, :] = jnp.concatenate([block(found, f), block(found, g), gap], axis=1)
        start_pairs(phase, near_pairs)

    def coefficients_of(phase, share, found, sign):
        for f in range(6):
            pl.when(exists[f])(tile_copy(phase, f, f).wait_recv)
        wait_pairs(phase, near_pairs)
        back = tile_in[phase, 0]
        for f in range(1, 6):
            back = back + tile_in[phase, f]
        own = share - sign * back[:, cases : 2 * cases]
        low = [None] * 6
        high = [None] * 6
        for index in near_pairs:
            a, b = pairs[index]
            tile = pair_in[phase, index, 0:padded]
            low[b] = tile if low[b] is None else low[b] + tile
            if a != b:
                high[a] = tile if high[a] is None else high[a] + tile
        terms = []
        for f in range(6):
            term = block(found, f)
            if low[f] is not None:
                term = term + low[f][:, 0:cases]
            if high[f] is not None:
                term = term + high[f][:, cases : 2 * cases]
            terms.append(tile_in[phase, f][:, 0:cases] - sign * term)
        wait_pairs(phase, far_pairs)
        for index in far_pairs:
            a, b = pairs[index]
            terms[b] = terms[b] - sign * pair_in[phase, index, 0:padded, 0:cases]
            terms[a] = terms[a] - sign * pair_in[phase, index, padded:, 0:cases]
        return jnp.concatenate([own, *terms, jnp.zeros((padded, cases), jnp.float32)], axis=0)

    def assembled(phase):
        return jnp.concatenate(
            [masked(value_out[phase, f] - value_in[phase, f], f) for f in range(6)], axis=1
        )

    def applied(values):
        head, tail = split(values)
        both = dot(jnp.concatenate([head, tail], axis=0), ordered[...])
        half = values.shape[0]
        return both[0:half] + both[half:]

    send_values(0)
    for f in range(6):
        start_if(exists[f], first_copy(f, f ^ 1))
    for d in range(3):
        start_if(exists[2 * d + 1], load_copy(d, 2 * d + 1))

    all_modes[0:padded, :] = mode_rows
    probes[6 * padded : 7 * padded, :] = inverse_modes
    fetches[5].wait()
    for d in range(3):
        low = 2 * d * width
        raw[pl.ds(low, width), :] = dot(narrow[d], raw[pl.ds(low, width), :]).astype(jnp.bfloat16)
    for d in range(3):
        low = 2 * d * width
        ordered[:, low : low + width] = lax.dot_general(
            raw[:, low : low + width], narrow[d], NT, preferred_element_type=jnp.float32
        ).astype(jnp.bfloat16)
        ordered[:, low + width : low + 2 * width] = raw[:, low + width : low + 2 * width]
    wait_values(0)
    for f in range(6):
        pl.when(exists[f])(first_copy(f, f).wait_recv)
    for f in range(6):
        span = slice(f * width, (f + 1) * width)
        all_modes[(1 + f) * padded : (2 + f) * padded, span] = first_in[f, 0:padded, :]
        probes[f * padded : (f + 1) * padded, span] = first_in[f, padded:, :]
    every_probe = split(probes[...])
    initial = assembled(0)
    product = applied(initial)
    for f in range(6):
        value_out[1, f] = face(product, f)
    send_values(1)
    for d in range(3):
        pl.when(exists[2 * d])(load_copy(d, 2 * d).wait_recv)
    right = []
    for d in range(3):
        right.append(masked(-load_in[d], 2 * d))
        right.append(masked(load_ref[:, d * width : (d + 1) * width], 2 * d + 1))
    right = jnp.concatenate(right, axis=1)
    found = fast(probes[...], product, NT)
    shares = fast(inverse_modes, right, NT) - block(found, 6)
    send_far(0, found)
    send_near(0, shares, found)
    every_mode = all_modes[...]
    images = applied(jnp.concatenate([every_mode, probes[...]], axis=0))
    depth = every_mode.shape[0]
    probe_image = images[depth:]
    mode_image = images[0:depth]
    cross_image = fast(probe_image, every_mode, NT)
    mode_stack = right_of(every_mode)
    image_stack = right_of(mode_image)
    head, tail = split(cross_image)
    folds = jnp.concatenate([head, head, tail], axis=1)

    def preconditioned(values, image, coefficients):
        left = left_of(0.25 * coefficients)
        return values - dot(left, mode_stack), image - dot(left, image_stack)

    wait_values(1)
    residual = right - assembled(1)
    product = applied(residual)
    probed = fast(probe_image, residual, NT)
    coefficients = coefficients_of(0, shares, found, -1.0)
    found = probed - dot(folds, right_of(0.25 * coefficients))
    start, product = preconditioned(residual, product, coefficients)
    for f in range(6):
        value_out[2, f] = face(product, f)
    send_lines(2)
    send_far(1, found)
    send_others(2)
    shares = block(found, 6)
    send_near(1, shares, found)

    relay = ny - 1
    is_relay = iy == relay

    def gathers(which, step):
        for offset in range(nx):
            other = lax.rem(nx - 1 - ix + offset, nx)
            copy = remote(
                plane_sums.at[which, slot],
                plane_sums.at[which, slot],
                plane_send.at[which, offset],
                plane_recv.at[which, slot],
                (other, relay, iz),
            )
            pl.when(jnp.logical_or(iy != relay, ix != other))(getattr(copy, step))

    def spreads(which, step):
        index = 0
        for turn in range(1, ny + 1):
            for offset in range(nz):
                level = jnp.where(2 * iz < nz, nz - 1 - offset, offset)
                copy = remote(
                    line_sums.at[which, iz],
                    line_sums.at[which, iz],
                    line_send.at[which, index],
                    line_recv.at[which, iz],
                    (ix, lax.rem(relay + turn, ny), level),
                )
                if turn < ny:
                    getattr(copy, step)()
                else:
                    pl.when(iz != level)(getattr(copy, step))
                index = index + 1

    def sum_start(which, tile):
        plane_sums[which, slot] = tile
        gathers(which, "start")

    def sum_middle(which):
        @pl.when(is_relay)
        def _():
            for other in range(plane):
                copy = remote(
                    plane_sums.at[which, other],
                    plane_sums.at[which, other],
                    plane_send.at[which, 0],
                    plane_recv.at[which, other],
                    (ix, iy, iz),
                )
                pl.when(slot != other)(copy.wait_recv)
            total = plane_sums[which, 0]
            for other in range(1, plane):
                total = total + plane_sums[which, other]
            line_sums[which, iz] = total
            spreads(which, "start")

    def sum_end(which):
        for other in range(nz):
            copy = remote(
                line_sums.at[which, other],
                line_sums.at[which, other],
                line_send.at[which, 0],
                line_recv.at[which, other],
                (ix, iy, iz),
            )
            pl.when(jnp.logical_or(iy != relay, iz != other))(copy.wait_recv)
        total = line_sums[which, 0]
        for other in range(1, nz):
            total = total + line_sums[which, other]
        half = total.shape[0] // 2
        return unpacked(total[0:half], cases), unpacked(total[half:], cases)

    def sum_finish(which):
        gathers(which, "wait_send")
        pl.when(is_relay)(functools.partial(spreads, which, "wait_send"))

    sum_start(
        0,
        jnp.concatenate(
            [
                packed(fast(owned(start), owned(residual), NT), width),
                packed(fast(start, product, NT), width),
            ],
            axis=0,
        ),
    )
    wait_values(2)
    image = assembled(2)
    product = applied(image)
    coefficients = coefficients_of(1, shares, found, 1.0)
    second, product = preconditioned(image, product, coefficients)
    sum_start(
        1,
        jnp.concatenate(
            [
                packed(fast(owned(second), owned(image), NT), width),
                packed(fast(second, product, NT), width),
            ],
            axis=0,
        ),
    )
    sum_middle(0)
    for f in range(6):
        value_out[3, f] = face(product, f)
    send_values(3)
    sum_middle(1)
    gram, energy = sum_end(0)
    inverse = eliminate(jnp.concatenate([energy, identity(cases)], axis=1), cases)
    alpha = fast(inverse, gram)
    starts = jnp.concatenate([owned(start), -owned(image)], axis=1)
    base = jnp.concatenate([owned(initial), owned(residual)], axis=1) + fast(alpha, starts, TN)
    wait_values(3)
    seconds = jnp.concatenate([owned(second), -owned(assembled(3))], axis=1)
    for condition, copy in sends:
        pl.when(condition)(copy.wait_send)
    sum_finish(0)
    cross, last = sum_end(1)
    carried = fast(inverse, cross)
    schur = last - fast(cross, carried)
    right_side = fast(cross, alpha) - energy
    tail = eliminate(jnp.concatenate([schur, right_side], axis=1), cases)
    steps = right_of(seconds - fast(carried, starts, TN))
    result = base - dot(left_of(tail), steps)
    multipliers_ref[...] = result[:, 0 : 3 * width]
    residual_ref[...] = result[:, 3 * width :]
    sum_finish(1)


def put_out(multipliers_ref, residual_ref, multipliers_hbm, residual_hbm, sem):
    copies = [
        pltpu.make_async_copy(multipliers_ref, multipliers_hbm, sem.at[0]),
        pltpu.make_async_copy(residual_ref, residual_hbm, sem.at[1]),
    ]
    for copy in copies:
        copy.start()
    for copy in copies:
        copy.wait()


def held(array):
    return pltpu.with_memory_space_constraint(array, pltpu.HBM)


def rows_apart(array):
    return jnp.swapaxes(array, 2, 3).reshape(array.shape[3], 1, array.shape[4])


def local(extents, dual_operators, dual_load, rigid_modes, coarse_load, mode_counts, face_maps):
    size = dual_operators.shape[-1]
    cases = dual_load.shape[-2]
    width = dual_load.shape[-1] // 3
    modes = rigid_modes.shape[-2]
    padded = -(-modes // 8) * 8
    nx, ny, nz = extents
    plane = nx * ny
    tile = 2 * cases // max(1, width // cases)
    f32 = jnp.float32
    vmem = pl.BlockSpec(memory_space=pltpu.VMEM)
    hbm = pl.BlockSpec(memory_space=pltpu.HBM)
    dma = pltpu.SemaphoreType.DMA
    out = jax.ShapeDtypeStruct((cases, 3 * width), f32)
    multipliers, residual = pl.pallas_call(
        functools.partial(kernel, extents),
        out_shape=(out, out),
        in_specs=[
            hbm,
            hbm,
            hbm,
            hbm,
            hbm,
            hbm,
        ],
        out_specs=(vmem, vmem),
        scratch_shapes=[
            pltpu.VMEM((size, size), dual_operators.dtype),
            pltpu.VMEM((cases, 3 * width), f32),
            pltpu.VMEM((modes, 1, size), f32),
            pltpu.VMEM((modes, 1, cases), f32),
            pltpu.VMEM((3, 1, width), jnp.int32),
            pltpu.VMEM((1, 1), jnp.int32),
            pltpu.VMEM((size, size), dual_operators.dtype),
            pltpu.VMEM((padded, size), f32),
            pltpu.VMEM((8 * padded, size), f32),
            pltpu.VMEM((padded, width), f32),
            pltpu.VMEM((8 * padded, size), f32),
            pltpu.VMEM((6, 2 * padded, width), f32),
            pltpu.VMEM((6, 2 * padded, width), f32),
            pltpu.VMEM((4, 6, cases, width), f32),
            pltpu.VMEM((4, 6, cases, width), f32),
            pltpu.VMEM((2, 6, padded, width), f32),
            pltpu.VMEM((2, 6, padded, width), f32),
            pltpu.VMEM((2, 18, 2 * padded, width), f32),
            pltpu.VMEM((2, 18, 2 * padded, width), f32),
            pltpu.VMEM((3, cases, width), f32),
            pltpu.VMEM((2, plane, tile, width), f32),
            pltpu.VMEM((2, nz, tile, width), f32),
            dma((6,)),
            dma((6,)),
            dma((6,)),
            dma((4, 6)),
            dma((4, 6)),
            dma((2, 6)),
            dma((2, 6)),
            dma((2, 18)),
            dma((2, 18)),
            dma((3,)),
            dma((3,)),
            dma((2, nx)),
            dma((2, plane)),
            dma((2, ny * nz)),
            dma((2, nz)),
        ],
        compiler_params=pltpu.CompilerParams(collective_id=0, has_side_effects=True, vmem_limit_bytes=16 * 1024 * 1024
        ),
    )(
        held(dual_operators.reshape(size, size)),
        held(dual_load.reshape(cases, 3 * width)),
        held(rows_apart(rigid_modes)),
        held(rows_apart(coarse_load)),
        mode_counts.reshape(1, 1),
        held(rows_apart(face_maps)),
    )
    multipliers, residual = pl.pallas_call(
        put_out,
        out_shape=(out, out),
        in_specs=[vmem, vmem],
        out_specs=(hbm, hbm),
        scratch_shapes=[dma((2,))],
        compiler_params=pltpu.CompilerParams(vmem_limit_bytes=1024 * 1024),
    )(multipliers, residual)
    shape = (1, 1, 1, cases, 3 * width)
    return multipliers.reshape(shape), residual.reshape(shape)


def solution(mesh):
    extents = (mesh.shape["gx"], mesh.shape["gy"], mesh.shape["gz"])
    spec = P("gx", "gy", "gz", None, None)
    return jax.shard_map(
        functools.partial(local, extents),
        mesh=mesh,
        in_specs=(spec, spec, spec, spec, P("gx", "gy", "gz"), spec),
        out_specs=(spec, spec),
        check_vma=False,
    )
```

```python
import functools

import jax
import jax.numpy as jnp
from jax import lax
from jax.experimental import pallas as pl
from jax.experimental.pallas import tpu as pltpu
from jax.sharding import PartitionSpec as P

MESH = pl.DeviceIdType.MESH
NN = (((1,), (0,)), ((), ()))
NT = (((1,), (1,)), ((), ()))
TN = (((0,), (0,)), ((), ()))


def split(a):
    head = a.astype(jnp.bfloat16)
    return head, (a - head.astype(jnp.float32)).astype(jnp.bfloat16)


def fast(a, b, dims=NN):
    if dims == TN:
        a, dims = a.T, NN
    (ah, al), (bh, bl) = split(a), split(b)
    dot = functools.partial(
        lax.dot_general, dimension_numbers=dims, preferred_element_type=jnp.float32
    )
    return dot(ah, bh) + (dot(ah, bl) + dot(al, bh))


def pivoted(entries, lines):
    span = range(len(lines))
    for j in span:
        scale = 1.0 / entries[j][j]
        lines[j] = lines[j] * scale
        scaled = [entries[j][q] * scale if q > j else None for q in span]
        for i in span:
            if i == j:
                continue
            factor = entries[min(i, j)][max(i, j)]
            for q in range(max(i, j + 1), len(lines)):
                entries[i][q] = entries[i][q] - factor * scaled[q]
            lines[i] = lines[i] - factor * lines[j]
        entries[j] = scaled
    return lines


def first_row(values, i):
    return pltpu.roll(values, values.shape[0] - i, 0)[0:1] if i else values[0:1]


def inverted(columns):
    span = range(len(columns))
    shape = (len(columns), 128)
    rows = lax.broadcasted_iota(jnp.int32, shape, 0)
    lanes = lax.broadcasted_iota(jnp.int32, (1, shape[1]), 1)
    wide = [jnp.broadcast_to(column, shape) for column in columns]
    entries = [[first_row(wide[q], i) if q >= i else None for q in span] for i in span]
    lines = pivoted(entries, [(lanes == i).astype(jnp.float32) for i in span])
    merged = jnp.broadcast_to(lines[0], shape)
    for i in span[1:]:
        merged = jnp.where(rows == i, jnp.broadcast_to(lines[i], shape), merged)
    return merged


def stacked(left, *right):
    (head, tail), (first, second) = split(left), split(jnp.concatenate(right, axis=0))
    dots = functools.partial(lax.dot_general, dimension_numbers=NT, preferred_element_type=jnp.float32)
    both = dots(jnp.concatenate([head, tail], axis=0), first)
    return both[0 : head.shape[0]] + (both[head.shape[0] :] + dots(head, second))


def eliminate(system, size, block=8):
    width = system.shape[1]
    shape = (block, width)
    rows = lax.broadcasted_iota(jnp.int32, shape, 0)
    panels = [system[p : p + block] for p in range(0, system.shape[0], block)]
    span = range(block)
    for k in range(0, size, block):
        pivot = panels[k // block]
        lines = [first_row(pivot, i) for i in span]
        entries = [
            [jnp.broadcast_to(lines[i][:, k + q : k + q + 1], (1, width)) if q >= i else None for q in span]
            for i in span
        ]
        columns = [
            [jnp.broadcast_to(panel[:, k + q : k + q + 1], shape) for q in span]
            for panel in panels
            if panel is not pivot
        ]
        lines = pivoted(entries, lines)
        lines = [jnp.broadcast_to(line, shape) for line in lines]
        merged = lines[0]
        for j in span[1:]:
            merged = jnp.where(rows == j, lines[j], merged)
        others = iter(columns)
        updated = []
        for panel in panels:
            if panel is pivot:
                updated.append(merged)
                continue
            column = next(others)
            update = column[0] * lines[0]
            for j in span[1:]:
                update = update + column[j] * lines[j]
            updated.append(panel - update)
        panels = updated
    return jnp.concatenate(panels, axis=0)[:, size:]


def identity(size):
    return (
        lax.broadcasted_iota(jnp.int32, (size, size), 0)
        == lax.broadcasted_iota(jnp.int32, (size, size), 1)
    ).astype(jnp.float32)


def packed(gram, width):
    groups = max(1, width // gram.shape[1])
    depth = gram.shape[0] // groups
    return jnp.concatenate([gram[g * depth : (g + 1) * depth] for g in range(groups)], axis=1)


def unpacked(tile, size):
    groups = max(1, tile.shape[1] // size)
    return jnp.concatenate([tile[:, g * size : (g + 1) * size] for g in range(groups)], axis=0)


def terms_of(left, right):
    total = left[:, 0:1] * right[0:1, :]
    for m in range(1, right.shape[0]):
        total = total + left[:, m : m + 1] * right[m : m + 1, :]
    return total


def thrice_rows(a):
    head = a.astype(jnp.bfloat16).astype(jnp.float32)
    return jnp.concatenate([head, head, a - head], axis=0)


def left_of(a):
    return thrice_rows(a).astype(jnp.bfloat16)


def right_of(a):
    head, tail = split(a)
    return jnp.concatenate([head, tail, head], axis=0)


def dot_tn(a, b):
    return lax.dot_general(a, b, TN, preferred_element_type=jnp.float32)


def dot(a, b):
    return jnp.dot(a, b, preferred_element_type=jnp.float32)


def kernel(
    extents,
    operator_hbm,
    load_hbm,
    modes_hbm,
    coarse_hbm,
    count_hbm,
    maps_hbm,
    multipliers_ref,
    residual_ref,
    raw,
    load_ref,
    modes_ref,
    coarse_ref,
    maps_ref,
    count_ref,
    ordered,
    own_modes,
    all_modes,
    padded_load,
    probes,
    first_out,
    first_in,
    value_out,
    value_in,
    tile_out,
    tile_in,
    pair_out,
    pair_in,
    load_in,
    plane_sums,
    line_sums,
    raw_sem,
    first_send,
    first_recv,
    value_send,
    value_recv,
    tile_send,
    tile_recv,
    pair_send,
    pair_recv,
    load_send,
    load_recv,
    plane_send,
    plane_recv,
    line_send,
    line_recv,
):
    nx, ny, nz = extents
    cases = load_hbm.shape[0]
    width = load_hbm.shape[1] // 3
    modes = modes_hbm.shape[0]
    padded = own_modes.shape[0]
    here = (lax.axis_index("gx"), lax.axis_index("gy"), lax.axis_index("gz"))
    ix, iy, iz = here
    plane = nx * ny
    slot = ix * ny + iy

    fetches = [
        pltpu.make_async_copy(source, target, raw_sem.at[i])
        for i, (source, target) in enumerate(
            (
                (modes_hbm, modes_ref),
                (count_hbm, count_ref),
                (coarse_hbm, coarse_ref),
                (maps_hbm, maps_ref),
                (load_hbm, load_ref),
                (operator_hbm, raw),
            )
        )
    ]
    for fetch in fetches:
        fetch.start()

    def plane_peer(offset):
        other = lax.rem(slot + offset, plane)
        return (lax.div(other, ny), lax.rem(other, ny), iz)

    def line_peers():
        for turn in range(ny):
            for offset in range(1, nz):
                yield (ix, lax.rem(iy + turn, ny), lax.rem(iz + offset, nz))

    exists = []
    neighbour = []
    for d in range(3):
        exists.append(here[d] > 0)
        exists.append(here[d] < extents[d] - 1)
        for step in (-1, 1):
            neighbour.append(tuple(here[a] + (step if a == d else 0) for a in range(3)))
    flags = [jnp.where(e, 1, 0).astype(jnp.int32) for e in exists]

    def moved(position, f):
        return tuple(position[a] + ((2 * (f % 2) - 1) if a == f // 2 else 0) for a in range(3))

    def both_exist(f, g):
        if f != g:
            return jnp.logical_and(exists[f], exists[g])
        if f % 2:
            return here[f // 2] < extents[f // 2] - 2
        return here[f // 2] > 1

    pairs = [
        (f, g)
        for f in range(6)
        for g in range(6)
        if (f == g or f // 2 < g // 2) and extents[f // 2] > 1 + (f == g) and extents[g // 2] > 1
    ]

    first_in[...] = jnp.zeros(first_in.shape, jnp.float32)
    pair_in[...] = jnp.zeros(pair_in.shape, jnp.float32)
    tile_in[...] = jnp.zeros(tile_in.shape, jnp.float32)

    barrier = pltpu.get_barrier_semaphore()
    def greet(peer):
        pl.semaphore_signal(barrier, inc=1, device_id=peer, device_id_type=MESH)

    expected = 0
    for f in range(6):
        pl.when(exists[f])(functools.partial(greet, neighbour[f]))
        expected = expected + flags[f]
    if max(nx, nz) + ny > 6:
        for f, g in pairs:
            pl.when(both_exist(f, g))(functools.partial(greet, moved(moved(here, f), g)))
            expected = expected + jnp.where(both_exist(f, g), 1, 0).astype(jnp.int32)
        for offset in range(1, plane):
            greet(plane_peer(offset))
        for peer in line_peers():
            greet(peer)
        expected = expected + (plane - 1 + ny * (nz - 1))

    all_modes[...] = jnp.zeros(all_modes.shape, jnp.float32)
    probes[...] = jnp.zeros(probes.shape, jnp.float32)
    own_modes[...] = jnp.zeros(own_modes.shape, jnp.float32)
    padded_load[...] = jnp.zeros(padded_load.shape, jnp.float32)

    def face(values, f):
        return values[:, f * width : (f + 1) * width]

    def masked(values, f):
        return jnp.where(jnp.full(values.shape, flags[f], jnp.int32) == 1, values, 0.0)

    def block(values, f):
        return values[f * padded : (f + 1) * padded]

    def remote(source, target, send, recv, where):
        return pltpu.make_async_remote_copy(
            src_ref=source,
            dst_ref=target,
            send_sem=send,
            recv_sem=recv,
            device_id=where,
            device_id_type=MESH,
        )

    def owned(values):
        return jnp.concatenate([face(values, 1), face(values, 3), face(values, 5)], axis=1)

    sends = []

    def start_if(condition, copy):
        pl.when(condition)(copy.start)
        sends.append((condition, copy))

    for fetch in fetches[:5]:
        fetch.wait()

    def counted(shape):
        return jnp.broadcast_to(count_ref[...], shape)

    lines = lax.broadcasted_iota(jnp.int32, (width, width), 0)
    narrow = [(lines == maps_ref[d]).astype(jnp.float32).astype(jnp.bfloat16) for d in range(3)]
    for m in range(modes):
        own_modes[m : m + 1, :] = modes_ref[m]
        padded_load[m : m + 1, 0:cases] = coarse_ref[m]
    raw_modes = jnp.where(
        lax.broadcasted_iota(jnp.int32, own_modes.shape, 0) < counted(own_modes.shape), own_modes[...], 0.0
    )
    raw_modes = jnp.concatenate([masked(face(raw_modes, f), f) for f in range(6)], axis=1)
    exact = []
    rest = raw_modes
    for _ in range(3):
        exact.append(rest.astype(jnp.bfloat16).astype(jnp.float32))
        rest = rest - exact[-1]
    exact = jnp.concatenate(exact, axis=0).astype(jnp.bfloat16)
    pieces = []
    for d in range(3):
        found = lax.dot_general(face(exact, 2 * d), narrow[d], NT, preferred_element_type=jnp.float32)
        pieces.append(found[0:padded] + found[padded : 2 * padded] + found[2 * padded :])
        pieces.append(face(raw_modes, 2 * d + 1))
    mode_rows = jnp.concatenate(pieces, axis=1)
    mode_index = lax.broadcasted_iota(jnp.int32, (padded, 1), 0)
    inactive = mode_index >= counted((padded, 1))
    columns = []
    for m in range(padded):
        column = jnp.sum(raw_modes * raw_modes[m : m + 1], axis=1, keepdims=True)
        columns.append(column + jnp.where(jnp.logical_and(inactive, mode_index == m), 1.0, 0.0))
    active_load = jnp.where(
        lax.broadcasted_iota(jnp.int32, padded_load.shape, 0) < counted(padded_load.shape), padded_load[...], 0.0
    )
    load_rows = active_load.T[0:cases]
    coarse_inverse = inverted(columns)
    inverse_modes = terms_of(coarse_inverse, mode_rows)
    spread = terms_of(load_rows, inverse_modes)
    for f in range(6):
        value_out[0, f] = face(spread, f)
        first_out[f, 0:padded, :] = -face(mode_rows, f)
        first_out[f, padded:, :] = face(inverse_modes, f)

    pl.semaphore_wait(barrier, expected)

    def value_copy(phase, f, landing):
        return remote(
            value_out.at[phase, f],
            value_in.at[phase, landing],
            value_send.at[phase, f],
            value_recv.at[phase, landing],
            neighbour[f],
        )

    def first_copy(f, landing):
        return remote(first_out.at[f], first_in.at[landing], first_send.at[f], first_recv.at[landing], neighbour[f])

    def load_copy(d, f):
        return remote(
            load_ref.at[:, pl.ds(d * width, width)],
            load_in.at[d],
            load_send.at[d],
            load_recv.at[d],
            neighbour[f],
        )

    def tile_copy(phase, f, landing):
        return remote(
            tile_out.at[phase, f],
            tile_in.at[phase, landing],
            tile_send.at[phase, f],
            tile_recv.at[phase, landing],
            neighbour[f],
        )

    far = [f != g and f < 2 and g >= 4 for f, g in pairs]

    def pair_part(ref, phase, index, wide):
        return ref.at[phase, index] if wide else ref.at[phase, index, pl.ds(0, padded)]

    def pair_copy(phase, index, landing):
        f, g = pairs[index]
        return remote(
            pair_part(pair_out, phase, index, far[index]),
            pair_part(pair_in, phase, landing, far[index]),
            pair_send.at[phase, index],
            pair_recv.at[phase, landing],
            moved(moved(here, f), g),
        )

    def start_pairs(phase, chosen):
        for index in chosen:
            f, g = pairs[index]
            start_if(both_exist(f, g), pair_copy(phase, index, pairs.index((f ^ 1, g ^ 1))))

    def wait_pairs(phase, chosen):
        for index in chosen:
            f, g = pairs[index]
            pl.when(both_exist(f, g))(pair_copy(phase, index, index).wait_recv)

    far_pairs = [index for index in range(len(pairs)) if far[index]]
    near_pairs = [index for index in range(len(pairs)) if not far[index]]

    def send_lines(phase):
        odd = lax.rem(ix, 2) == 1
        even = jnp.logical_not(odd)
        for f, turn in ((1, odd), (0, even), (0, odd), (1, even)):
            start_if(jnp.logical_and(exists[f], turn), value_copy(phase, f, f ^ 1))

    def send_others(phase):
        for f in (4, 5, 2, 3):
            start_if(exists[f], value_copy(phase, f, f ^ 1))

    def send_values(phase):
        send_lines(phase)
        send_others(phase)

    def wait_values(phase):
        for f in range(6):
            pl.when(exists[f])(value_copy(phase, f, f).wait_recv)

    def send_far(phase, found):
        for index in far_pairs:
            f, g = pairs[index]
            pair_out[phase, index, 0:padded, 0:cases] = block(found, f)
            pair_out[phase, index, padded:, 0:cases] = block(found, g)
        start_pairs(phase, far_pairs)

    def send_near(phase, share, found):
        gap = jnp.zeros((padded, width - 2 * cases), jnp.float32)
        for f in range(6):
            tile_out[phase, f] = jnp.concatenate([share, block(found, f), gap], axis=1)
        for f in range(6):
            start_if(exists[f], tile_copy(phase, f, f ^ 1))
        for index in near_pairs:
            f, g = pairs[index]
            if f == g:
                pair_out[phase, index, 0:padded, 0:cases] = block(found, f)
            else:
                pair_out[phase, index, 0:padded, :] = jnp.concatenate([block(found, f), block(found, g), gap], axis=1)
        start_pairs(phase, near_pairs)

    def coefficients_of(phase, share, found, sign):
        for f in range(6):
            pl.when(exists[f])(tile_copy(phase, f, f).wait_recv)
        wait_pairs(phase, near_pairs)
        back = tile_in[phase, 0]
        for f in range(1, 6):
            back = back + tile_in[phase, f]
        own = share - sign * back[:, cases : 2 * cases]
        low = [None] * 6
        high = [None] * 6
        for index in near_pairs:
            a, b = pairs[index]
            tile = pair_in[phase, index, 0:padded]
            low[b] = tile if low[b] is None else low[b] + tile
            if a != b:
                high[a] = tile if high[a] is None else high[a] + tile
        terms = []
        for f in range(6):
            term = block(found, f)
            if low[f] is not None:
                term = term + low[f][:, 0:cases]
            if high[f] is not None:
                term = term + high[f][:, cases : 2 * cases]
            terms.append(tile_in[phase, f][:, 0:cases] - sign * term)
        wait_pairs(phase, far_pairs)
        for index in far_pairs:
            a, b = pairs[index]
            terms[b] = terms[b] - sign * pair_in[phase, index, 0:padded, 0:cases]
            terms[a] = terms[a] - sign * pair_in[phase, index, padded:, 0:cases]
        return jnp.concatenate([own, *terms, jnp.zeros((padded, cases), jnp.float32)], axis=0)

    def assembled(phase):
        return jnp.concatenate(
            [masked(value_out[phase, f] - value_in[phase, f], f) for f in range(6)], axis=1
        )

    def applied(values):
        head, tail = split(values)
        both = dot(jnp.concatenate([head, tail], axis=0), ordered[...])
        half = values.shape[0]
        return both[0:half] + both[half:]

    send_values(0)
    for f in range(6):
        start_if(exists[f], first_copy(f, f ^ 1))
    for d in range(3):
        start_if(exists[2 * d + 1], load_copy(d, 2 * d + 1))

    all_modes[0:padded, :] = mode_rows
    probes[6 * padded : 7 * padded, :] = inverse_modes
    fetches[5].wait()
    for d in range(3):
        low = 2 * d * width
        raw[pl.ds(low, width), :] = dot(narrow[d], raw[pl.ds(low, width), :]).astype(jnp.bfloat16)
    for d in range(3):
        low = 2 * d * width
        ordered[:, low : low + width] = lax.dot_general(
            raw[:, low : low + width], narrow[d], NT, preferred_element_type=jnp.float32
        ).astype(jnp.bfloat16)
        ordered[:, low + width : low + 2 * width] = raw[:, low + width : low + 2 * width]
    wait_values(0)
    for f in range(6):
        pl.when(exists[f])(first_copy(f, f).wait_recv)
    for f in range(6):
        span = slice(f * width, (f + 1) * width)
        all_modes[(1 + f) * padded : (2 + f) * padded, span] = first_in[f, 0:padded, :]
        probes[f * padded : (f + 1) * padded, span] = first_in[f, padded:, :]
    every_probe = split(probes[...])
    initial = assembled(0)
    product = applied(initial)
    for f in range(6):
        value_out[1, f] = face(product, f)
    send_values(1)
    for d in range(3):
        pl.when(exists[2 * d])(load_copy(d, 2 * d).wait_recv)
    right = []
    for d in range(3):
        right.append(masked(-load_in[d], 2 * d))
        right.append(masked(load_ref[:, d * width : (d + 1) * width], 2 * d + 1))
    right = jnp.concatenate(right, axis=1)
    found = fast(probes[...], product, NT)
    shares = fast(inverse_modes, right, NT) - block(found, 6)
    send_far(0, found)
    send_near(0, shares, found)
    every_mode = all_modes[...]
    images = applied(jnp.concatenate([every_mode, probes[...]], axis=0))
    depth = every_mode.shape[0]
    probe_image = images[depth:]
    mode_image = images[0:depth]
    cross_image = fast(probe_image, every_mode, NT)
    mode_stack = right_of(every_mode)
    image_stack = right_of(mode_image)
    head, tail = split(cross_image)
    folds = jnp.concatenate([head, head, tail], axis=1)

    def preconditioned(values, image, coefficients):
        left = left_of(0.25 * coefficients)
        return values - dot_tn(left, mode_stack), image - dot_tn(left, image_stack)

    wait_values(1)
    residual = right - assembled(1)
    product = applied(residual)
    probed = fast(probe_image, residual, NT)
    coefficients = coefficients_of(0, shares, found, -1.0)
    found = probed - dot(folds, right_of(0.25 * coefficients))
    start, product = preconditioned(residual, product, coefficients)
    for f in range(6):
        value_out[2, f] = face(product, f)
    send_lines(2)
    send_far(1, found)
    send_others(2)
    shares = block(found, 6)
    send_near(1, shares, found)

    relay = ny - 1
    is_relay = iy == relay

    def gathers(which, step):
        for offset in range(nx):
            other = lax.rem(nx - 1 - ix + offset, nx)
            copy = remote(
                plane_sums.at[which, slot],
                plane_sums.at[which, slot],
                plane_send.at[which, offset],
                plane_recv.at[which, slot],
                (other, relay, iz),
            )
            pl.when(jnp.logical_or(iy != relay, ix != other))(getattr(copy, step))

    def spreads(which, step):
        index = 0
        for turn in range(1, ny + 1):
            for offset in range(nz):
                level = jnp.where(2 * iz < nz, nz - 1 - offset, offset)
                copy = remote(
                    line_sums.at[which, iz],
                    line_sums.at[which, iz],
                    line_send.at[which, index],
                    line_recv.at[which, iz],
                    (ix, lax.rem(relay + turn, ny), level),
                )
                if turn < ny:
                    getattr(copy, step)()
                else:
                    pl.when(iz != level)(getattr(copy, step))
                index = index + 1

    def sum_start(which, tile):
        plane_sums[which, slot] = tile
        gathers(which, "start")

    def sum_middle(which):
        @pl.when(is_relay)
        def _():
            for other in range(plane):
                copy = remote(
                    plane_sums.at[which, other],
                    plane_sums.at[which, other],
                    plane_send.at[which, 0],
                    plane_recv.at[which, other],
                    (ix, iy, iz),
                )
                pl.when(slot != other)(copy.wait_recv)
            total = plane_sums[which, 0]
            for other in range(1, plane):
                total = total + plane_sums[which, other]
            line_sums[which, iz] = total
            spreads(which, "start")

    def sum_end(which):
        for other in range(nz):
            copy = remote(
                line_sums.at[which, other],
                line_sums.at[which, other],
                line_send.at[which, 0],
                line_recv.at[which, other],
                (ix, iy, iz),
            )
            pl.when(jnp.logical_or(iy != relay, iz != other))(copy.wait_recv)
        total = line_sums[which, 0]
        for other in range(1, nz):
            total = total + line_sums[which, other]
        half = total.shape[0] // 2
        return unpacked(total[0:half], cases), unpacked(total[half:], cases)

    def sum_finish(which):
        gathers(which, "wait_send")
        pl.when(is_relay)(functools.partial(spreads, which, "wait_send"))

    sum_start(
        0,
        jnp.concatenate(
            [
                packed(fast(owned(start), owned(residual), NT), width),
                packed(fast(start, product, NT), width),
            ],
            axis=0,
        ),
    )
    wait_values(2)
    image = assembled(2)
    product = applied(image)
    coefficients = coefficients_of(1, shares, found, 1.0)
    second, product = preconditioned(image, product, coefficients)
    masked_image = jnp.concatenate(
        [face(image, f) if f % 2 else jnp.zeros((cases, width), jnp.float32) for f in range(6)], axis=1
    )
    both = stacked(second, masked_image, product)
    sum_start(
        1, jnp.concatenate([packed(both[:, 0:cases], width), packed(both[:, cases:], width)], axis=0)
    )
    sum_middle(0)
    for f in range(6):
        value_out[3, f] = face(product, f)
    send_values(3)
    sum_middle(1)
    gram, energy = sum_end(0)
    inverse = eliminate(jnp.concatenate([energy, identity(cases)], axis=1), cases)
    alpha = fast(inverse, gram)
    starts = jnp.concatenate([owned(start), -owned(image)], axis=1)
    base = jnp.concatenate([owned(initial), owned(residual)], axis=1) + fast(alpha, starts, TN)
    wait_values(3)
    seconds = jnp.concatenate([owned(second), -owned(assembled(3))], axis=1)
    for condition, copy in sends:
        pl.when(condition)(copy.wait_send)
    sum_finish(0)
    cross, last = sum_end(1)
    carried = fast(inverse, cross)
    schur = last - fast(cross, carried)
    right_side = fast(cross, alpha) - energy
    tail = eliminate(jnp.concatenate([schur, right_side], axis=1), cases)
    steps = right_of(seconds - fast(carried, starts, TN))
    result = base - dot_tn(left_of(tail), steps)
    multipliers_ref[...] = result[:, 0 : 3 * width]
    residual_ref[...] = result[:, 3 * width :]
    sum_finish(1)


def put_out(multipliers_ref, residual_ref, multipliers_hbm, residual_hbm, sem):
    copies = [
        pltpu.make_async_copy(multipliers_ref, multipliers_hbm, sem.at[0]),
        pltpu.make_async_copy(residual_ref, residual_hbm, sem.at[1]),
    ]
    for copy in copies:
        copy.start()
    for copy in copies:
        copy.wait()


def held(array):
    return pltpu.with_memory_space_constraint(array, pltpu.HBM)


def rows_apart(array):
    return jnp.swapaxes(array, 2, 3).reshape(array.shape[3], 1, array.shape[4])


def local(extents, dual_operators, dual_load, rigid_modes, coarse_load, mode_counts, face_maps):
    size = dual_operators.shape[-1]
    cases = dual_load.shape[-2]
    width = dual_load.shape[-1] // 3
    modes = rigid_modes.shape[-2]
    padded = -(-modes // 8) * 8
    nx, ny, nz = extents
    plane = nx * ny
    tile = 2 * cases // max(1, width // cases)
    f32 = jnp.float32
    vmem = pl.BlockSpec(memory_space=pltpu.VMEM)
    hbm = pl.BlockSpec(memory_space=pltpu.HBM)
    dma = pltpu.SemaphoreType.DMA
    out = jax.ShapeDtypeStruct((cases, 3 * width), f32)
    multipliers, residual = pl.pallas_call(
        functools.partial(kernel, extents),
        out_shape=(out, out),
        in_specs=[
            hbm,
            hbm,
            hbm,
            hbm,
            hbm,
            hbm,
        ],
        out_specs=(vmem, vmem),
        scratch_shapes=[
            pltpu.VMEM((size, size), dual_operators.dtype),
            pltpu.VMEM((cases, 3 * width), f32),
            pltpu.VMEM((modes, 1, size), f32),
            pltpu.VMEM((modes, 1, cases), f32),
            pltpu.VMEM((3, 1, width), jnp.int32),
            pltpu.VMEM((1, 1), jnp.int32),
            pltpu.VMEM((size, size), dual_operators.dtype),
            pltpu.VMEM((padded, size), f32),
            pltpu.VMEM((8 * padded, size), f32),
            pltpu.VMEM((padded, width), f32),
            pltpu.VMEM((8 * padded, size), f32),
            pltpu.VMEM((6, 2 * padded, width), f32),
            pltpu.VMEM((6, 2 * padded, width), f32),
            pltpu.VMEM((4, 6, cases, width), f32),
            pltpu.VMEM((4, 6, cases, width), f32),
            pltpu.VMEM((2, 6, padded, width), f32),
            pltpu.VMEM((2, 6, padded, width), f32),
            pltpu.VMEM((2, 18, 2 * padded, width), f32),
            pltpu.VMEM((2, 18, 2 * padded, width), f32),
            pltpu.VMEM((3, cases, width), f32),
            pltpu.VMEM((2, plane, tile, width), f32),
            pltpu.VMEM((2, nz, tile, width), f32),
            dma((6,)),
            dma((6,)),
            dma((6,)),
            dma((4, 6)),
            dma((4, 6)),
            dma((2, 6)),
            dma((2, 6)),
            dma((2, 18)),
            dma((2, 18)),
            dma((3,)),
            dma((3,)),
            dma((2, nx)),
            dma((2, plane)),
            dma((2, ny * nz)),
            dma((2, nz)),
        ],
        compiler_params=pltpu.CompilerParams(collective_id=0, has_side_effects=True, vmem_limit_bytes=16 * 1024 * 1024
        ),
    )(
        held(dual_operators.reshape(size, size)),
        held(dual_load.reshape(cases, 3 * width)),
        held(rows_apart(rigid_modes)),
        held(rows_apart(coarse_load)),
        mode_counts.reshape(1, 1),
        held(rows_apart(face_maps)),
    )
    multipliers, residual = pl.pallas_call(
        put_out,
        out_shape=(out, out),
        in_specs=[vmem, vmem],
        out_specs=(hbm, hbm),
        scratch_shapes=[dma((2,))],
        compiler_params=pltpu.CompilerParams(vmem_limit_bytes=1024 * 1024),
    )(multipliers, residual)
    shape = (1, 1, 1, cases, 3 * width)
    return multipliers.reshape(shape), residual.reshape(shape)


def solution(mesh):
    extents = (mesh.shape["gx"], mesh.shape["gy"], mesh.shape["gz"])
    spec = P("gx", "gy", "gz", None, None)
    return jax.shard_map(
        functools.partial(local, extents),
        mesh=mesh,
        in_specs=(spec, spec, spec, spec, P("gx", "gy", "gz"), spec),
        out_specs=(spec, spec),
        check_vma=False,
    )
```
